256 devices in a mesh: seq: 32 (over z, y), mp: 8 (over x, core).
Axes of the slice: x: 4, y: 4, z: 8, core: 2. Of those that a mesh axis runs over, the one named last changes fastest.
Arguments:
- ssm_input: bfloat16 [32768, 5120], P('seq', 'mp'), may hold values from -6 to 6
- gate_input: bfloat16 [32768, 5120], P('seq', 'mp'), may hold values from -6 to 6
- state_in: bfloat16 [32768, 128], P('seq'), may hold values from -6 to 6
- state_out: bfloat16 [32768, 128], P('seq'), may hold values from -0.5 to 0.5
- step_size: float32 [32768, 80], P('seq', 'mp'), may hold values from 0.05 to 0.2
- log_decay: float32 [32768, 80], P('seq', 'mp'), may hold values from -2 to 0
- skip_gain: float32 [80], P('mp'), may hold values from 0.5 to 2
- norm_gain: bfloat16 [5120], P('mp'), may hold values from 0.099609375 to 1.8984375
- out_weight: bfloat16 [5120, 2560], P('mp'), may hold values from -0.078125 to 0.078125
Outputs:
- layer_out: bfloat16 [32768, 2560], P(('seq', 'mp'))
The draws below stay inside these ranges and needn't reach their ends.
All inputs are finite; a program needn't handle non-finite values.
Results may differ from the reference program's by a relative error of at most 0.011.
Values may be sent and summed in bfloat16 or wider, within the bound.
No kernel may reach another device: no remote copies, remote signals or barrier semaphores. Data moves between devices by JAX's collectives and lax.ppermute only.
A program may use at most 64 MiB of HBM per device.

```python
import math
import jax
import jax.numpy as jnp
from jax import lax

D = 2560
HEAD_TOTAL = 80
HEAD_DIM = 64
STATE = 128
BLOCK = 256
TOK_DEV = 1024
TOKEN_TOTAL = 32768
INNER = 5120


def draw_log_decay(key, part):
    sequence_lanes = jax.random.split(key, 6)
    slow_share = 0.5
    chooser = jax.random.uniform(sequence_lanes[0], (HEAD_TOTAL,))
    fast_rate = jnp.exp(jax.random.uniform(sequence_lanes[1], (HEAD_TOTAL,), minval=jnp.log(1.0 / 60.0), maxval=jnp.log(1.0 / 25.0)))
    slow_rate = jnp.exp(jax.random.uniform(sequence_lanes[2], (HEAD_TOTAL,), minval=jnp.log(0.03), maxval=jnp.log(0.2))) / TOKEN_TOTAL
    head_decay_rates = jnp.where(chooser < slow_share, slow_rate, fast_rate)
    device_count = TOKEN_TOTAL // TOK_DEV
    shard_multiplier = jnp.exp(jax.random.uniform(sequence_lanes[3], (device_count, 1), minval=0.0, maxval=jnp.log(3.0)))
    shard_multiplier = jnp.repeat(shard_multiplier, TOK_DEV, axis=0)
    jaggedness = jnp.exp(jax.random.uniform(sequence_lanes[4], (TOKEN_TOTAL, HEAD_TOTAL), minval=jnp.log(0.5), maxval=jnp.log(2.0)))
    spike_locations = jax.random.randint(sequence_lanes[5], (2,), 0, TOKEN_TOTAL)
    spike_retain = jax.random.uniform(jax.random.fold_in(key, 7), (2, HEAD_TOTAL), minval=0.5, maxval=0.8)
    token_offsets = jnp.arange(TOKEN_TOTAL)[:, None]
    spike_events = jnp.where(token_offsets == spike_locations[0], jnp.log(spike_retain[0])[None, :], 0.0)
    spike_events = spike_events + jnp.where(token_offsets == spike_locations[1], jnp.log(spike_retain[1])[None, :], 0.0)
    return (-(head_decay_rates[None, :] * shard_multiplier * jaggedness) + spike_events).astype(jnp.float32)


def shard_levels(rng, extent, shards, least, largest):
    gain = 1.0
    for dim, shards_of in shards:
        draws = jax.random.uniform(jax.random.fold_in(jax.random.fold_in(rng, 6), dim), (shards_of,), jnp.float32, least / len(shards), largest / len(shards))
        gain = gain * jnp.repeat(jnp.exp(draws), extent[dim] // shards_of).reshape((-1,) + (1,) * (len(extent) - 1 - dim))
    return gain


def centred(own_key, dims, deviation, reach, pieces=(), dtype=jnp.bfloat16):
    loudness = shard_levels(own_key, dims, pieces, -0.22, 0.18) if pieces else 1.0
    drawn = jax.random.normal(own_key, dims, jnp.float32) * deviation * loudness
    return jnp.minimum(jnp.maximum(drawn, -reach), reach).astype(dtype)


def setup_inputs(seed: int = 0) -> dict:
    arg_keys = jax.random.split(jax.random.key(seed), 10)
    ssm_input = centred(arg_keys[0], (TOKEN_TOTAL, INNER), 1.0, 6.0, ((0, 32), (1, 8)))
    gate_input = centred(arg_keys[1], (TOKEN_TOTAL, INNER), 1.0, 6.0, ((0, 32), (1, 8)))
    state_in = centred(arg_keys[2], (TOKEN_TOTAL, STATE), 1.0, 6.0, ((0, 32),))
    state_out = centred(arg_keys[3], (TOKEN_TOTAL, STATE), STATE ** -0.5, 0.5, ((0, 32),))
    step_size = jnp.clip(jnp.exp(math.log(0.2) - 1.3862944 * jax.random.uniform(arg_keys[4], (TOKEN_TOTAL, HEAD_TOTAL), jnp.float32) ** shard_levels(arg_keys[4], (TOKEN_TOTAL, HEAD_TOTAL), ((0, 32), (1, 8)), -0.2, 0.2)), 0.05, 0.2)
    log_decay = draw_log_decay(jax.random.fold_in(arg_keys[9], 71), 0)
    skip_gain = jnp.clip(0.5 + 1.5 * jax.random.uniform(arg_keys[6], (HEAD_TOTAL,), jnp.float32) ** shard_levels(arg_keys[6], (HEAD_TOTAL,), ((0, 8),), -0.2, 0.2), 0.5, 2.0)
    norm_gain = jnp.clip(1.0 + 0.18 * jax.random.normal(arg_keys[7], (INNER,), jnp.float32), 0.099609375, 1.8984375).astype(jnp.bfloat16)
    out_weight = centred(arg_keys[8], (INNER, D), INNER ** -0.5, 0.078125, ((0, 8),))
    return dict(ssm_input=ssm_input, gate_input=gate_input, state_in=state_in, state_out=state_out, step_size=step_size, log_decay=log_decay, skip_gain=skip_gain, norm_gain=norm_gain, out_weight=out_weight)


def reference(ssm_input, gate_input, state_in, state_out, step_size, log_decay, skip_gain, norm_gain, out_weight):
    blocks = TOKEN_TOTAL // BLOCK
    inputs = ssm_input.reshape(blocks, BLOCK, HEAD_TOTAL, HEAD_DIM)
    gates = gate_input.reshape(blocks, BLOCK, INNER)
    writers = state_in.reshape(blocks, BLOCK, STATE)
    readers = state_out.reshape(blocks, BLOCK, STATE)
    steps_all = step_size.reshape(blocks, BLOCK, HEAD_TOTAL)
    decays_all = log_decay.reshape(blocks, BLOCK, HEAD_TOTAL)
    causal = jnp.arange(BLOCK)[:, None] >= jnp.arange(BLOCK)[None, :]
    gain_wide = norm_gain.astype(jnp.float32)

    def one_block(state, packed):
        inp, gate, writer, reader, steps, decay = packed
        level = jnp.cumsum(decay, axis=0)
        level_t = level.T
        intersection = jnp.dot(reader, writer.T, preferred_element_type=jnp.float32)
        gaps = level_t[:, :, None] - level_t[:, None, :]
        decays = jnp.where(causal[None], jnp.exp(jnp.where(causal[None], gaps, 0.0)), 0.0)
        score = (decays * intersection[None] * steps.T[:, None, :]).astype(jnp.bfloat16)
        within = jnp.einsum('hts,shp->thp', score.astype(jnp.float32), inp.astype(jnp.float32))
        from_carry = jnp.exp(level)[:, :, None] * jnp.einsum('tn,hpn->thp', reader.astype(jnp.float32), state, precision=lax.Precision.HIGHEST)
        closing = level[-1]
        weighted = ((jnp.exp(closing[None, :] - level) * steps)[:, :, None] * inp.astype(jnp.float32)).astype(jnp.bfloat16)
        own_state = jnp.einsum('shp,sn->hpn', weighted.astype(jnp.float32), writer.astype(jnp.float32))
        new_state = jnp.exp(closing)[:, None, None] * state + own_state
        mixed = within + from_carry + skip_gain[None, :, None] * inp.astype(jnp.float32)
        gated = mixed.reshape(BLOCK, INNER) * jax.nn.silu(gate.astype(jnp.float32))
        mean_sq = lax.optimization_barrier(jnp.mean(gated * gated, axis=1, keepdims=True))
        normed = (gated * lax.rsqrt(mean_sq + 1e-05) * gain_wide[None, :]).astype(jnp.bfloat16)
        result = jnp.dot(normed, out_weight, preferred_element_type=jnp.float32).astype(jnp.bfloat16)
        return (new_state, result)
    start = jnp.zeros((HEAD_TOTAL, HEAD_DIM, STATE), jnp.float32)
    final_state, results = lax.scan(one_block, start, (inputs, gates, writers, readers, steps_all, decays_all))
    return results.reshape(TOKEN_TOTAL, D)
```

```python
import jax
import jax.numpy as jnp
from jax import lax
from jax.experimental import pallas as pl
from jax.experimental.pallas import tpu as pltpu
from jax.sharding import Mesh
from jax.sharding import PartitionSpec as P

BLOCK = 256
HALF = 128
HEADS = 10
WIDTH = 64
CH = HEADS * WIDTH
STATE = 128
ROWS = 1024
NBLK = ROWS // BLOCK
SEQ_DEV = 32
PIECE = STATE // SEQ_DEV
D = 2560
DH = D // 2
PADH = 16
LOG2E = 1.4426950408889634
F32 = jnp.float32
BF16 = jnp.bfloat16


def parts(value, count):
    out = []
    for _ in range(count):
        piece = value.astype(BF16)
        out.append(piece)
        value = value - piece.astype(F32)
    return out


def spread_matrix(count, tail):
    cols = CH + (HALF if tail else 0)
    row = lax.broadcasted_iota(jnp.int32, (PADH * count, cols), 0) % PADH
    col = lax.broadcasted_iota(jnp.int32, (PADH * count, cols), 1)
    head = jnp.where(col < CH, col // WIDTH, col - CH)
    return jnp.where(row == head, 1.0, 0.0).astype(BF16)


def spread(value, matrix, count):
    stacked = jnp.concatenate(parts(value, count), axis=0)
    return lax.dot_general(stacked, matrix, (((0,), (0,)), ((), ())), preferred_element_type=F32)


def state_kernel(x_ref, b_ref, dt_ref, ld_ref, msg_ref, early_ref, lev_ref, lead_ref, pad_ref, dtp_ref, run_ref):
    pad_ref[...] = jnp.zeros_like(pad_ref)
    dtp_ref[...] = jnp.zeros_like(dtp_ref)
    dtp_ref[0:HEADS, :] = dt_ref[...]
    for k in range(NBLK):
        pad_ref[PADH * k : PADH * k + HEADS, :] = ld_ref[:, BLOCK * k : BLOCK * (k + 1)]
    upper = jnp.where(
        lax.broadcasted_iota(jnp.int32, (BLOCK, BLOCK), 0) <= lax.broadcasted_iota(jnp.int32, (BLOCK, BLOCK), 1),
        1.0,
        0.0,
    ).astype(BF16)
    stacked = jnp.concatenate(parts(pad_ref[...], 3), axis=0)
    sums = jnp.dot(stacked, upper, preferred_element_type=F32)
    rows = PADH * NBLK
    levels = sums[0:rows] + sums[rows : 2 * rows] + sums[2 * rows : 3 * rows]
    lane = lax.broadcasted_iota(jnp.int32, (PADH, HALF), 1)
    table = jnp.zeros((PADH, HALF), F32)
    total = jnp.zeros((PADH, 1), F32)
    for k in range(NBLK):
        lev = levels[PADH * k : PADH * (k + 1)]
        lev_ref[:, BLOCK * k : BLOCK * (k + 1)] = lev
        closing = lev[:, BLOCK - 1 : BLOCK]
        table = jnp.where(lane == k, jnp.exp(closing), table)
        table = jnp.where(lane == 8 + k, jnp.exp(total), table)
        total = total + closing
    table = jnp.where(lane == 4, total, table)
    wide = spread(table, spread_matrix(3, True), 3)
    lead_ref[...] = wide[8:16, 0:CH]
    two = spread_matrix(2, False)
    for k in range(NBLK):
        lev = levels[PADH * k : PADH * (k + 1)]
        closing = lev[:, BLOCK - 1 : BLOCK]
        weight = jnp.exp(closing - lev) * dtp_ref[:, BLOCK * k : BLOCK * (k + 1)]
        weighted = (spread(weight, two, 2) * x_ref[BLOCK * k : BLOCK * (k + 1), :].astype(F32)).astype(BF16)
        own = lax.dot_general(
            b_ref[BLOCK * k : BLOCK * (k + 1), :], weighted, (((0,), (0,)), ((), ())), preferred_element_type=F32
        )
        if k == 0:
            early_ref[k] = jnp.zeros((STATE, CH), BF16)
            run_ref[...] = own
        else:
            early_ref[k] = run_ref[...].astype(BF16)
            run_ref[...] = wide[k : k + 1, 0:CH] * run_ref[...] + own
    decay = wide[4:5, CH : CH + HALF]
    decays = jnp.concatenate([v.astype(F32) for v in parts(decay, 3)] + [jnp.zeros((1, HALF), F32)], axis=0)
    decays = decays.astype(BF16)
    for q in range(SEQ_DEV):
        msg_ref[q, :, 0:CH] = run_ref[PIECE * q : PIECE * (q + 1), :].astype(BF16)
        msg_ref[q, :, CH : CH + HALF] = decays


def prefix_kernel(msg_ref, out_ref, dec_ref):
    for i in range(SEQ_DEV):
        for part in range(3):
            dec_ref[part, i : i + 1, :] = msg_ref[i, :, CH : CH + HALF].astype(F32)[part : part + 1]
    head = lax.broadcasted_iota(jnp.int32, (HALF, CH), 0)
    col = lax.broadcasted_iota(jnp.int32, (HALF, CH), 1)
    matrix = jnp.where(head == col // WIDTH, 1.0, 0.0).astype(BF16)
    logs = jnp.zeros((SEQ_DEV, CH), F32)
    for part in range(3):
        logs = logs + jnp.dot(dec_ref[part].astype(BF16), matrix, preferred_element_type=F32)
    decay = jnp.exp(logs)
    running = jnp.zeros((PIECE, CH), F32)
    for i in range(SEQ_DEV):
        out_ref[i] = running.astype(BF16)
        running = decay[i : i + 1, :] * running + msg_ref[i, :, 0:CH].astype(F32)


def local_kernel(x_ref, g_ref, b_ref, c_ref, dt_ref, lev_ref, early_ref, lead_ref, skip_ref, gl_ref, fs_ref):
    k = pl.program_id(0)
    lev = lev_ref[...]
    lev2 = lev * LOG2E
    cols = jnp.transpose(lev2)
    rows = lev2[0:HEADS] - jnp.log(dt_ref[...]) * LOG2E
    reader, writer = c_ref[...], b_ref[...]
    inter = lax.dot_general(reader, writer, (((1,), (1,)), ((), ())), preferred_element_type=F32)
    causal = lax.broadcasted_iota(jnp.int32, (HALF, HALF), 0) >= lax.broadcasted_iota(jnp.int32, (HALF, HALF), 1)
    lane = lax.broadcasted_iota(jnp.int32, (HALF, HALF), 1) < WIDTH
    grown = spread(jnp.exp(lev), spread_matrix(2, False), 2)
    carry = jnp.dot(reader, early_ref[0], preferred_element_type=F32)

    def score(head, r, s):
        gap = cols[HALF * r : HALF * (r + 1), head : head + 1] - rows[head : head + 1, HALF * s : HALF * (s + 1)]
        value = jnp.exp2(gap) * inter[HALF * r : HALF * (r + 1), HALF * s : HALF * (s + 1)]
        if r == s:
            value = jnp.where(causal, value, 0.0)
        return value.astype(BF16)

    lead = jnp.sum(jnp.where(lax.broadcasted_iota(jnp.int32, (8, CH), 0) == k, lead_ref[...], 0.0), axis=0, keepdims=True)
    for pair in range(HEADS // 2):
        lanes = slice(HALF * pair, HALF * (pair + 1))
        top_x = x_ref[0:HALF, lanes]
        low_x = x_ref[HALF:BLOCK, lanes]
        tops, lows = [], []
        for head in (2 * pair, 2 * pair + 1):
            tops.append(jnp.dot(score(head, 0, 0), top_x, preferred_element_type=F32))
            lows.append(
                jnp.dot(score(head, 1, 0), top_x, preferred_element_type=F32)
                + jnp.dot(score(head, 1, 1), low_x, preferred_element_type=F32)
            )
        for r, (even, odd), x_part in ((0, tops, top_x), (1, lows, low_x)):
            span = slice(HALF * r, HALF * (r + 1))
            mixed = (
                jnp.where(lane, even, odd)
                + grown[span, lanes] * carry[span, lanes]
                + skip_ref[:, lanes] * x_part.astype(F32)
            )
            gate = g_ref[span, lanes].astype(F32)
            gate = gate / (1.0 + jnp.exp(-gate))
            gl_ref[span, lanes] = mixed * gate
            fs_ref[span, lanes] = grown[span, lanes] * lead[:, lanes] * gate


def gate_kernel(
    idx_ref, p_ref, gain_ref, cs_ref, ck_ref, gls_ref, glk_ref, fss_ref, fsk_ref, send_ref, keep_ref, sqs_ref, sqk_ref, st_ref
):
    @pl.when(pl.program_id(0) == 0)
    def _():
        for q in range(SEQ_DEV):
            st_ref[PIECE * q : PIECE * (q + 1), :] = p_ref[q].astype(F32)

    state = st_ref[...].astype(BF16)
    for reader, local, factor, out, square in (
        (cs_ref, gls_ref, fss_ref, send_ref, sqs_ref),
        (ck_ref, glk_ref, fsk_ref, keep_ref, sqk_ref),
    ):
        gated = local[...] + factor[...] * jnp.dot(reader[...], state, preferred_element_type=F32)
        sums = jnp.sum(gated * gated, axis=1, keepdims=True)
        square[0] = jnp.transpose(jnp.broadcast_to(sums, (HALF, HALF)))[0:8, :]
        out[...] = (gated * gain_ref[...]).astype(BF16)


def product_kernel(own_ref, other_ref, wo_ref, wp_ref, out_ref):
    value = jnp.dot(own_ref[...], wo_ref[...], preferred_element_type=F32)
    value = value + jnp.dot(other_ref[...], wp_ref[...], preferred_element_type=F32)
    out_ref[...] = value.astype(out_ref.dtype)


def cost(flops, read):
    return pl.CostEstimate(flops=int(flops), bytes_accessed=int(read), transcendentals=0)


def whole(shape):
    return pl.BlockSpec(shape, lambda *_: (0,) * len(shape))


def local_state(x, b, dt, ld):
    return pl.pallas_call(
        state_kernel,
        out_shape=(
            jax.ShapeDtypeStruct((SEQ_DEV, PIECE, CH + HALF), BF16),
            jax.ShapeDtypeStruct((NBLK, STATE, CH), BF16),
            jax.ShapeDtypeStruct((PADH, ROWS), F32),
            jax.ShapeDtypeStruct((8, CH), F32),
        ),
        scratch_shapes=[
            pltpu.VMEM((PADH * NBLK, BLOCK), F32),
            pltpu.VMEM((PADH, ROWS), F32),
            pltpu.VMEM((STATE, CH), F32),
        ],
        cost_estimate=cost(4e8, 3e6),
        name="local_state",
    )(x, b, dt, ld)


def seq_prefix(msg):
    return pl.pallas_call(
        prefix_kernel,
        out_shape=jax.ShapeDtypeStruct((SEQ_DEV, PIECE, CH), BF16),
        scratch_shapes=[pltpu.VMEM((3, SEQ_DEV, HALF), F32)],
        name="seq_prefix",
    )(msg)


def local_part(x, g, b, c, dt, lev, early, lead, skip):
    rows = lambda width: pl.BlockSpec((BLOCK, width), lambda k: (k, 0))
    return pl.pallas_call(
        local_kernel,
        grid=(NBLK,),
        in_specs=[
            rows(CH),
            rows(CH),
            rows(STATE),
            rows(STATE),
            pl.BlockSpec((HEADS, BLOCK), lambda k: (0, k)),
            pl.BlockSpec((PADH, BLOCK), lambda k: (0, k)),
            pl.BlockSpec((1, STATE, CH), lambda k: (k, 0, 0)),
            whole((8, CH)),
            whole((1, CH)),
        ],
        out_specs=(rows(CH), rows(CH)),
        out_shape=(jax.ShapeDtypeStruct((ROWS, CH), F32), jax.ShapeDtypeStruct((ROWS, CH), F32)),
        cost_estimate=cost(2e9, 1e7),
        name="local_part",
    )(x, g, b, c, dt, lev, early, lead, skip)


def gated_rows(order, prefix, gain, c, gl, fs):
    count = order.shape[0] - 1
    send = lambda width: pl.BlockSpec((HALF, width), lambda i, idx: (2 * idx[i + 1] + 1 - idx[0], 0))
    keep = lambda width: pl.BlockSpec((HALF, width), lambda i, idx: (2 * idx[i + 1] + idx[0], 0))
    out = pl.BlockSpec((HALF, CH), lambda i, idx: (i, 0))
    square = pl.BlockSpec((1, 8, HALF), lambda i, idx: (i, 0, 0))
    return pl.pallas_call(
        gate_kernel,
        grid_spec=pltpu.PrefetchScalarGridSpec(
            num_scalar_prefetch=1,
            grid=(count,),
            in_specs=[
                pl.BlockSpec((SEQ_DEV, PIECE, CH), lambda i, idx: (0, 0, 0)),
                pl.BlockSpec((1, CH), lambda i, idx: (0, 0)),
                send(STATE),
                keep(STATE),
                send(CH),
                keep(CH),
                send(CH),
                keep(CH),
            ],
            out_specs=(out, out, square, square),
            scratch_shapes=[pltpu.VMEM((STATE, CH), F32)],
        ),
        out_shape=(
            jax.ShapeDtypeStruct((HALF * count, CH), BF16),
            jax.ShapeDtypeStruct((HALF * count, CH), BF16),
            jax.ShapeDtypeStruct((count, 8, HALF), F32),
            jax.ShapeDtypeStruct((count, 8, HALF), F32),
        ),
        cost_estimate=cost(1e8 * count, 2e6 * count),
        name="gated_rows",
    )(order, prefix, gain, c, c, gl, gl, fs, fs)


def product(own, other, row, w_own, w_other, first, cols, dtype):
    tile = 640
    start = first // tile
    return pl.pallas_call(
        product_kernel,
        grid=(cols // tile,),
        in_specs=[
            pl.BlockSpec((HALF, CH), lambda j: (row, 0)),
            pl.BlockSpec((HALF, CH), lambda j: (row, 0)),
            pl.BlockSpec((CH, tile), lambda j: (0, start + j)),
            pl.BlockSpec((CH, tile), lambda j: (0, start + j)),
        ],
        out_specs=pl.BlockSpec((HALF, tile), lambda j: (0, j)),
        out_shape=jax.ShapeDtypeStruct((HALF, cols), dtype),
        cost_estimate=cost(4 * HALF * CH * cols, 4 * CH * cols),
        name="product",
    )(own, other, w_own, w_other)


def body(x, g, b, c, dt, ld, skip, gain, w):
    chips = lax.axis_size("x")
    chip, core = lax.axis_index("x"), lax.axis_index("c")
    up = [(i, (i + 1) % chips) for i in range(chips)]
    down = [(i, (i - 1) % chips) for i in range(chips)]
    swap = [(0, 1), (1, 0)]
    w_other = lax.ppermute(w, "c", swap)
    msg, early, lev, lead = local_state(x, b, dt.T, ld.T)
    msg = lax.all_to_all(msg, ("z", "y"), split_axis=0, concat_axis=0, tiled=True)
    skip_wide = jnp.repeat(skip, WIDTH)[None, :]
    gl, fs = local_part(x, g, b, c, dt.T, lev, early, lead, skip_wide)
    prefix = lax.all_to_all(seq_prefix(msg), ("z", "y"), split_axis=0, concat_axis=0, tiled=True)
    gain_row = gain.astype(F32)[None, :]
    far, right, left = (chip + 2) % chips, (chip + 1) % chips, (chip + 3) % chips
    order = lambda *blocks: jnp.stack([core, *blocks]).astype(jnp.int32)
    send0, keep0, sqs0, sqk0 = gated_rows(order(far), prefix, gain_row, c, gl, fs)
    got0 = lax.ppermute(send0, "c", swap)
    send1, keep1, sqs1, sqk1 = gated_rows(order(right, left, chip), prefix, gain_row, c, gl, fs)
    got1 = lax.ppermute(send1, "c", swap)
    far_a = lax.ppermute(product(keep0, got0, 0, w, w_other, 0, DH, BF16), "x", up)
    far_b = lax.ppermute(product(keep0, got0, 0, w, w_other, DH, DH, BF16), "x", down)
    right_b = lax.ppermute(product(keep1, got1, 0, w, w_other, DH, DH, BF16), "x", up)
    left_a = lax.ppermute(product(keep1, got1, 1, w, w_other, 0, DH, BF16), "x", down)
    right_a = product(keep1, got1, 0, w, w_other, 0, DH, F32)
    left_b = product(keep1, got1, 1, w, w_other, DH, DH, F32)
    right_a = lax.ppermute((right_a + far_a.astype(F32)).astype(BF16), "x", up)
    left_b = lax.ppermute((left_b + far_b.astype(F32)).astype(BF16), "x", down)
    own = product(keep1, got1, 2, w, w_other, 0, D, F32)

    squares_send = jnp.concatenate([sqs0, sqs1], axis=0)[:, 0]
    squares_keep = jnp.concatenate([sqk0, sqk1], axis=0)[:, 0]
    place = jnp.stack([far, right, left, chip])
    table = jnp.zeros((2 * chips, HALF), F32)
    table = table.at[2 * place + 1 - core].set(squares_send).at[2 * place + core].set(squares_keep)
    table = lax.all_to_all(table[:, None, :], ("x", "c"), split_axis=0, concat_axis=0, tiled=True)
    scale = lax.rsqrt(jnp.sum(table, axis=(0, 1)) / (CH * 2 * chips) + 1e-05)[:, None]
    half_a = own[:, :DH] + right_a.astype(F32) + left_a.astype(F32)
    half_b = own[:, DH:] + right_b.astype(F32) + left_b.astype(F32)
    return (jnp.concatenate([half_a, half_b], axis=1) * scale).astype(BF16)


def solution(mesh):
    torus = Mesh(mesh.devices.reshape(8, 4, 4, 2), ("z", "y", "x", "c"))
    seq, mp = ("z", "y"), ("x", "c")
    in_specs = (
        P(seq, mp),
        P(seq, mp),
        P(seq, None),
        P(seq, None),
        P(seq, mp),
        P(seq, mp),
        P(mp),
        P(mp),
        P(mp, None),
    )
    return jax.shard_map(body, mesh=torus, in_specs=in_specs, out_specs=P(seq + mp, None), check_vma=False)
```

```python
import functools

import jax
import jax.numpy as jnp
from jax import lax
from jax.experimental import pallas as pl
from jax.experimental.pallas import tpu as pltpu
from jax.sharding import Mesh
from jax.sharding import PartitionSpec as P


BLOCK = 256
HALF = 128
HEADS = 10
WIDTH = 64
CH = HEADS * WIDTH
STATE = 128
ROWS = 1024
NBLK = ROWS // BLOCK
SEQ_DEV = 32
PIECE = STATE // SEQ_DEV
D = 2560
DH = D // 2
PADH = 16
TALL = HALF + 8
LOG2E = 1.4426950408889634
F32 = jnp.float32
BF16 = jnp.bfloat16


def parts(value, count):
    out = []
    for _ in range(count):
        piece = value.astype(BF16)
        out.append(piece)
        value = value - piece.astype(F32)
    return out


def spread_matrix(count, tail):
    cols = CH + (HALF if tail else 0)
    row = lax.broadcasted_iota(jnp.int32, (PADH * count, cols), 0) % PADH
    col = lax.broadcasted_iota(jnp.int32, (PADH * count, cols), 1)
    head = jnp.where(col < CH, col // WIDTH, col - CH)
    return jnp.where(row == head, 1.0, 0.0).astype(BF16)


def spread(value, matrix, count):
    stacked = jnp.concatenate(parts(value, count), axis=0)
    return lax.dot_general(stacked, matrix, (((0,), (0,)), ((), ())), preferred_element_type=F32)


def triangle():
    row = lax.broadcasted_iota(jnp.int32, (BLOCK, BLOCK), 0)
    return jnp.where(row <= lax.broadcasted_iota(jnp.int32, (BLOCK, BLOCK), 1), 1.0, 0.0).astype(BF16)


def running_sums(value):
    rows = value.shape[0]
    sums = jnp.dot(jnp.concatenate(parts(value, 3), axis=0), triangle(), preferred_element_type=F32)
    return sums[0:rows] + sums[rows : 2 * rows] + sums[2 * rows : 3 * rows]


def state_kernel(
    x_hbm, b_hbm, dt_hbm, ld_hbm, msg_ref, pad_ref, dtp_ref, run_ref, x_ref, b_ref, dt_ref, ld_ref, sem
):
    copies = [pltpu.make_async_copy(ld_hbm, ld_ref, sem.at[0]), pltpu.make_async_copy(dt_hbm, dt_ref, sem.at[1])]
    for k in range(NBLK):
        rows = pl.ds(BLOCK * k, BLOCK)
        copies.append(pltpu.make_async_copy(x_hbm.at[rows, :], x_ref.at[rows, :], sem.at[2 + 2 * k]))
        copies.append(pltpu.make_async_copy(b_hbm.at[rows, :], b_ref.at[rows, :], sem.at[3 + 2 * k]))
    for copy in copies:
        copy.start()
    pad_ref[...] = jnp.zeros_like(pad_ref)
    dtp_ref[...] = jnp.zeros_like(dtp_ref)
    copies[0].wait()
    for k in range(NBLK):
        pad_ref[PADH * k : PADH * k + HEADS, :] = ld_ref[:, BLOCK * k : BLOCK * (k + 1)]
    levels = running_sums(pad_ref[...])
    closings = [levels[PADH * k : PADH * (k + 1), BLOCK - 1 : BLOCK] for k in range(NBLK)]
    tails = [jnp.zeros((PADH, 1), F32)]
    for k in reversed(range(NBLK)):
        tails.insert(0, tails[0] + closings[k])
    lane = lax.broadcasted_iota(jnp.int32, (PADH, HALF), 1)
    decay = spread(jnp.where(lane == 0, tails[0], 0.0), spread_matrix(3, True)[:, CH:], 3)[0:1, :]
    decays = jnp.concatenate([v.astype(F32) for v in parts(decay, 3)] + [jnp.zeros((1, HALF), F32)], axis=0)
    decays = decays.astype(BF16)
    two = spread_matrix(2, False)
    copies[1].wait()
    dtp_ref[0:HEADS, :] = dt_ref[...]
    total = None
    for k in range(NBLK):
        weight = jnp.exp(tails[k] - levels[PADH * k : PADH * (k + 1)]) * dtp_ref[:, BLOCK * k : BLOCK * (k + 1)]
        wide = spread(weight, two, 2)
        copies[2 + 2 * k].wait()
        copies[3 + 2 * k].wait()
        weighted = (wide * x_ref[BLOCK * k : BLOCK * (k + 1), :].astype(F32)).astype(BF16)
        own = lax.dot_general(
            b_ref[BLOCK * k : BLOCK * (k + 1), :], weighted, (((0,), (0,)), ((), ())), preferred_element_type=F32
        )
        total = own if total is None else total + own
    run_ref[...] = total
    for q in range(SEQ_DEV):
        msg_ref[q, :, 0:CH] = run_ref[PIECE * q : PIECE * (q + 1), :].astype(BF16)
        msg_ref[q, :, CH : CH + HALF] = decays


def prefix_kernel(msg_ref, out_ref, dec_ref):
    for i in range(SEQ_DEV):
        for part in range(3):
            dec_ref[part, i : i + 1, :] = msg_ref[i, :, CH : CH + HALF].astype(F32)[part : part + 1]
    head = lax.broadcasted_iota(jnp.int32, (HALF, CH), 0)
    col = lax.broadcasted_iota(jnp.int32, (HALF, CH), 1)
    matrix = jnp.where(head == col // WIDTH, 1.0, 0.0).astype(BF16)
    logs = jnp.zeros((SEQ_DEV, CH), F32)
    for part in range(3):
        logs = logs + jnp.dot(dec_ref[part].astype(BF16), matrix, preferred_element_type=F32)
    decay = jnp.exp(logs)
    running = jnp.zeros((PIECE, CH), F32)
    for i in range(SEQ_DEV):
        out_ref[i] = running.astype(BF16)
        running = decay[i : i + 1, :] * running + msg_ref[i, :, 0:CH].astype(F32)


def local_kernel(x_ref, g_ref, b_ref, c_ref, dt_ref, ld_ref, skip_ref, gl_ref, fs_ref, run_ref, lead_ref, pad_ref, dtp_ref):
    k = pl.program_id(0)

    @pl.when(k == 0)
    def _():
        run_ref[...] = jnp.zeros_like(run_ref)
        lead_ref[...] = jnp.zeros_like(lead_ref)
        pad_ref[...] = jnp.zeros_like(pad_ref)
        dtp_ref[...] = jnp.zeros_like(dtp_ref)

    pad_ref[0:HEADS, :] = ld_ref[...]
    dtp_ref[0:HEADS, :] = dt_ref[...]
    lev = running_sums(pad_ref[...])
    closing = lev[:, BLOCK - 1 : BLOCK]
    reader, writer = c_ref[...], b_ref[...]
    two = spread_matrix(2, False)
    lane = lax.broadcasted_iota(jnp.int32, (PADH, HALF), 1)
    table = jnp.where(lane == 0, jnp.exp(lead_ref[...]), jnp.where(lane == 1, jnp.exp(closing), 0.0))
    table = spread(table, spread_matrix(3, False), 3)
    lead = table[0:1, :]
    lead_ref[...] += closing
    grown = spread(jnp.exp(lev), two, 2)
    carry = jnp.dot(reader, run_ref[...].astype(BF16), preferred_element_type=F32)
    weight = spread(jnp.exp(closing - lev) * dtp_ref[...], two, 2)
    weighted = (weight * x_ref[...].astype(F32)).astype(BF16)
    own = lax.dot_general(writer, weighted, (((0,), (0,)), ((), ())), preferred_element_type=F32)
    run_ref[...] = table[1:2, :] * run_ref[...] + own
    lev2 = lev * LOG2E
    cols = jnp.transpose(lev2)
    rows = lev2[0:HEADS] - jnp.log(dt_ref[...]) * LOG2E
    inter = lax.dot_general(reader, writer, (((1,), (1,)), ((), ())), preferred_element_type=F32)
    causal = lax.broadcasted_iota(jnp.int32, (HALF, HALF), 0) >= lax.broadcasted_iota(jnp.int32, (HALF, HALF), 1)
    lane = lax.broadcasted_iota(jnp.int32, (HALF, HALF), 1) < WIDTH

    def score(head, r, s):
        gap = cols[HALF * r : HALF * (r + 1), head : head + 1] - rows[head : head + 1, HALF * s : HALF * (s + 1)]
        value = jnp.exp2(gap) * inter[HALF * r : HALF * (r + 1), HALF * s : HALF * (s + 1)]
        if r == s:
            value = jnp.where(causal, value, 0.0)
        return value.astype(BF16)

    for pair in range(HEADS // 2):
        lanes = slice(HALF * pair, HALF * (pair + 1))
        top_x = x_ref[0:HALF, lanes]
        low_x = x_ref[HALF:BLOCK, lanes]
        tops, lows = [], []
        for head in (2 * pair, 2 * pair + 1):
            tops.append(jnp.dot(score(head, 0, 0), top_x, preferred_element_type=F32))
            lows.append(
                jnp.dot(score(head, 1, 0), top_x, preferred_element_type=F32)
                + jnp.dot(score(head, 1, 1), low_x, preferred_element_type=F32)
            )
        for r, (even, odd), x_part in ((0, tops, top_x), (1, lows, low_x)):
            span = slice(HALF * r, HALF * (r + 1))
            mixed = (
                jnp.where(lane, even, odd)
                + grown[span, lanes] * carry[span, lanes]
                + skip_ref[:, lanes] * x_part.astype(F32)
            )
            gate = g_ref[span, lanes].astype(F32)
            gate = gate / (1.0 + jnp.exp(-gate))
            out_rows = pl.ds(pl.multiple_of(k * BLOCK + HALF * r, HALF), HALF)
            gl_ref[out_rows, lanes] = (mixed * gate).astype(BF16)
            fs_ref[out_rows, lanes] = (grown[span, lanes] * lead[:, lanes] * gate).astype(BF16)


def square_rows(total):
    rows = [piece.astype(F32) for piece in parts(total, 3)]
    return jnp.concatenate(rows + [jnp.zeros((8 - len(rows), HALF), F32)], axis=0).astype(BF16)


def squares_of(ref, first):
    return jnp.sum(ref[first : first + 8, 0:HALF].astype(F32), axis=0, keepdims=True)


def gate_kernel(first, count, idx_ref, p_ref, gain_ref, c_ref, gl_ref, fs_ref, *rest):
    fetch = None
    if len(rest) > 2:
        w_hbm, rows_ref, square_ref, p_out_ref, w_ref, st_ref, sem = rest
        fetch = pltpu.make_async_copy(w_hbm.at[:, 0:DH], w_ref, sem.at[0])
        fetch.start()
        for q in range(SEQ_DEV):
            st_ref[PIECE * q : PIECE * (q + 1), :] = p_ref[q].astype(F32)
        state = st_ref[...].astype(BF16)
        p_out_ref[...] = state
    else:
        rows_ref, square_ref = rest
        state = p_ref[...]
    gain = gain_ref[...]
    squares = []
    for side, half in enumerate((1 - idx_ref[0], idx_ref[0])):
        for i in range(count):
            rows = pl.ds(pl.multiple_of((2 * idx_ref[first + i] + half) * HALF, HALF), HALF)
            gated = gl_ref[rows, :].astype(F32) + fs_ref[rows, :].astype(F32) * jnp.dot(
                c_ref[rows, :], state, preferred_element_type=F32
            )
            sums = jnp.sum(gated * gated, axis=1, keepdims=True)
            squares.append(jnp.transpose(jnp.broadcast_to(sums, (HALF, HALF)))[0:1, :])
            place = count * side + i
            rows_ref[HALF * place : HALF * (place + 1), :] = (gated * gain).astype(BF16)
    square_ref[...] = jnp.concatenate(squares + [jnp.zeros((8 - len(squares), HALF), F32)], axis=0)
    if fetch is not None:
        fetch.wait()


def put_squares(ref, base, total):
    ref[base : base + TALL - HALF, 0:HALF] = square_rows(total)
    ref[base : base + TALL - HALF, HALF:DH] = jnp.zeros((TALL - HALF, DH - HALF), BF16)


def product_kernel(rows_ref, square_ref, w_ref, *rest):
    fetch = None
    if len(rest) > 2:
        w_hbm, send_ref, keep_ref, w_next_ref, sem = rest
        fetch = pltpu.make_async_copy(w_hbm.at[:, DH:D], w_next_ref, sem.at[0])
        fetch.start()
    else:
        send_ref, keep_ref = rest
    count = rows_ref.shape[0] // (2 * HALF)
    tall = send_ref.shape[0] // count
    rows = rows_ref[...]
    for j in range(DH // BLOCK):
        cols = slice(BLOCK * j, BLOCK * (j + 1))
        value = jnp.dot(rows, w_ref[:, cols], preferred_element_type=F32)
        keep_ref[:, cols] = value[HALF * count : 2 * HALF * count]
        for i in range(count):
            send_ref[tall * i : tall * i + HALF, cols] = value[HALF * i : HALF * (i + 1)].astype(BF16)
    if tall == TALL:
        for i in range(count):
            put_squares(send_ref, tall * i + HALF, square_ref[i : i + 1, :])
    if fetch is not None:
        fetch.wait()


def join_kernel(place, keep_ref, got_ref, *refs):
    out_ref = refs[-1]
    count = keep_ref.shape[0] // HALF
    tall = got_ref.shape[0] // count
    value = keep_ref[HALF * place : HALF * (place + 1), :] + got_ref[tall * place : tall * place + HALF, :].astype(F32)
    squares = tall == TALL
    more = refs[squares:-1]
    for ref in more:
        value = value + ref[0:HALF, :].astype(F32)
    out_ref[0:HALF, :] = value.astype(BF16)
    if squares:
        total = refs[0][count + place : count + place + 1, :] + squares_of(got_ref, tall * place + HALF)
        for ref in more:
            total = total + squares_of(ref, HALF)
        put_squares(out_ref, HALF, total)


def finish_kernel(devices, square_ref, ka_ref, kb_ref, ga_ref, gb_ref, ra_ref, la_ref, rb_ref, lb_ref, out_ref, scale_ref):
    rows = out_ref.shape[0]
    count = ka_ref.shape[0] // HALF
    last = count - 1

    @pl.when(pl.program_id(0) == 0)
    def _():
        total = square_ref[count + last : count + last + 1, :] + squares_of(ga_ref, TALL * last + HALF)
        total = total + squares_of(ra_ref, HALF) + squares_of(la_ref, HALF)
        scale = lax.rsqrt(total / (CH * devices) + 1e-05)
        scale_ref[...] = jnp.transpose(jnp.broadcast_to(scale, (HALF, HALF)))

    def part(ref, tall):
        return ref[pl.ds(pl.multiple_of(pl.program_id(0) * rows + tall * last, 8), rows), :].astype(F32)

    span = pl.ds(pl.multiple_of(pl.program_id(0) * rows, rows), rows)
    scale = scale_ref[span, 0:1]
    for i, (keep, got, tall, one, two) in enumerate(
        ((ka_ref, ga_ref, TALL, ra_ref, la_ref), (kb_ref, gb_ref, HALF, rb_ref, lb_ref))
    ):
        value = part(keep, HALF) + part(got, tall) + one[span, :].astype(F32) + two[span, :].astype(F32)
        out_ref[:, DH * i : DH * (i + 1)] = (value * scale).astype(BF16)


VMEM = pl.BlockSpec(memory_space=pltpu.VMEM)
SMEM = pl.BlockSpec(memory_space=pltpu.SMEM)
HBM = pl.BlockSpec(memory_space=pltpu.HBM)
LIMIT = 24 * 1024 * 1024


def local_call(kernel, args, outs, scratch=(), flops=1e8, in_specs=None, out_specs=None):
    in_specs, out_specs = in_specs or [VMEM] * len(args), out_specs or [VMEM] * len(outs)
    args = [pltpu.with_memory_space_constraint(v, pltpu.HBM) if spec is HBM else v for v, spec in zip(args, in_specs)]
    return pl.pallas_call(
        kernel,
        in_specs=in_specs,
        out_specs=out_specs,
        out_shape=[
            pltpu.HBM(*out) if spec is HBM else jax.ShapeDtypeStruct(*out) for out, spec in zip(outs, out_specs)
        ],
        scratch_shapes=[pltpu.VMEM(*v) if isinstance(v, tuple) else pltpu.SemaphoreType.DMA((v,)) for v in scratch],
        cost_estimate=pl.CostEstimate(flops=int(flops), bytes_accessed=0, transcendentals=0),
        compiler_params=pltpu.CompilerParams(vmem_limit_bytes=LIMIT),
    )(*args)


def local_state(x, b, dt, ld):
    outs = (((SEQ_DEV, PIECE, CH + HALF), BF16),)
    scratch = [
        ((PADH * NBLK, BLOCK), F32),
        ((PADH, ROWS), F32),
        ((STATE, CH), F32),
        ((ROWS, CH), BF16),
        ((ROWS, STATE), BF16),
        ((HEADS, ROWS), F32),
        ((HEADS, ROWS), F32),
        2 + 2 * NBLK,
    ]
    return local_call(state_kernel, (x, b, dt, ld), outs, scratch, 1e9, [HBM] * 4)[0]


def seq_prefix(msg):
    outs = (((SEQ_DEV, PIECE, CH), BF16),)
    scratch = [((3, SEQ_DEV, HALF), F32)]
    return local_call(prefix_kernel, (msg,), outs, scratch)[0]


def whole(shape):
    return pl.BlockSpec(shape, lambda *_: (0,) * len(shape))


def local_part(x, g, b, c, dt, ld, skip):
    rows = lambda width: pl.BlockSpec((BLOCK, width), lambda k: (k, 0))
    heads = pl.BlockSpec((HEADS, BLOCK), lambda k: (0, k))
    return pl.pallas_call(
        local_kernel,
        grid=(NBLK,),
        in_specs=[rows(CH), rows(CH), rows(STATE), rows(STATE), heads, heads, whole((1, CH))],
        out_specs=(VMEM, VMEM),
        out_shape=(jax.ShapeDtypeStruct((ROWS, CH), BF16), jax.ShapeDtypeStruct((ROWS, CH), BF16)),
        scratch_shapes=[
            pltpu.VMEM((STATE, CH), F32),
            pltpu.VMEM((PADH, HALF), F32),
            pltpu.VMEM((PADH, BLOCK), F32),
            pltpu.VMEM((PADH, BLOCK), F32),
        ],
        cost_estimate=pl.CostEstimate(flops=int(3e9), bytes_accessed=0, transcendentals=0),
        compiler_params=pltpu.CompilerParams(vmem_limit_bytes=LIMIT),
        name="local_part",
    )(*(pltpu.with_memory_space_constraint(v, pltpu.HBM) for v in (x, g, b, c, dt, ld)), skip)


def gated_rows(order, first, count, prefix, gain, c, gl, fs, *w):
    outs = [((2 * HALF * count, CH), BF16), ((8, HALF), F32)]
    scratch = []
    in_specs = [SMEM] + [VMEM] * 5 + [HBM] * len(w)
    if w:
        outs += [((STATE, CH), BF16), ((CH, DH), BF16)]
        scratch = [((STATE, CH), F32), 1]
    kernel = functools.partial(gate_kernel, first, count)
    return local_call(kernel, (order, prefix, gain, c, gl, fs, *w), outs, scratch, 5e8 * count, in_specs)


def product(rows, squares, w, tall, *w_next):
    count = rows.shape[0] // (2 * HALF)
    outs = [((tall * count, DH), BF16), ((HALF * count, DH), F32)] + [((CH, DH), BF16)] * len(w_next)
    in_specs = [VMEM] * 3 + [HBM] * len(w_next)
    flops = 2 * rows.shape[0] * CH * DH
    return local_call(product_kernel, (rows, squares, w, *w_next), outs, [1] * len(w_next), flops, in_specs)


def join(place, keep, got, *more):
    tall = got.shape[0] * HALF // keep.shape[0]
    return local_call(functools.partial(join_kernel, place), (keep, got, *more), (((tall, DH), BF16),))[0]


def finish(devices, *args):
    rows = 32
    return pl.pallas_call(
        functools.partial(finish_kernel, devices),
        grid=(HALF // rows,),
        in_specs=[VMEM] * len(args),
        out_specs=pl.BlockSpec((rows, D), lambda i: (i, 0)),
        out_shape=jax.ShapeDtypeStruct((HALF, D), BF16),
        scratch_shapes=[pltpu.VMEM((HALF, HALF), F32)],
        compiler_params=pltpu.CompilerParams(vmem_limit_bytes=LIMIT),
        name="finish",
    )(*args)


def after(value, earlier):
    return lax.optimization_barrier((value, earlier))[0]


def body(x, g, b, c, dt, ld, skip, gain, w):
    chips = lax.axis_size("x")
    chip, core = lax.axis_index("x"), lax.axis_index("c")
    up = [(i, (i + 1) % chips) for i in range(chips)]
    down = [(i, (i - 1) % chips) for i in range(chips)]
    swap = [(0, 1), (1, 0)]
    far, right, left = (chip + 2) % chips, (chip + 1) % chips, (chip + 3) % chips
    order = jnp.stack([core, far, right, left, chip]).astype(jnp.int32)
    msg = local_state(x, b, dt.T, ld.T)
    msg = lax.all_to_all(msg, ("z", "y"), split_axis=0, concat_axis=0, tiled=True)
    skip_wide = jnp.repeat(skip, WIDTH)[None, :]
    gl, fs = local_part(x, g, b, c, dt.T, ld.T, skip_wide)
    prefix = lax.all_to_all(seq_prefix(msg), ("z", "y"), split_axis=0, concat_axis=0, tiled=True)
    gain_row = gain.astype(F32)[None, :]

    rows0, square0, prefix, w_a = gated_rows(order, 1, 1, prefix, gain_row, c, gl, fs, w)
    send_a, keep_a, w_b = product(rows0, square0, w_a, TALL, w)
    got_a = lax.ppermute(send_a, "c", swap)
    send_b, keep_b = product(after(rows0, send_a), square0, w_b, HALF)
    got_b = lax.ppermute(send_b, "c", swap)
    rows1, square1 = gated_rows(order, 2, 3, after(prefix, send_b), gain_row, c, gl, fs)
    far_a = join(0, after(keep_a, rows1), got_a, square0)
    far_b = join(0, after(keep_b, far_a), got_b)
    rows1 = after(rows1, far_b)
    far_a, far_b = lax.ppermute(far_a, "x", up), lax.ppermute(far_b, "x", down)
    send_b, keep_b = product(rows1, square1, w_b, HALF)
    got_b = lax.ppermute(send_b, "c", swap)
    send_a, keep_a = product(after(rows1, send_b), square1, w_a, TALL)
    got_a = lax.ppermute(send_a, "c", swap)
    right_b = join(0, after(keep_b, send_a), got_b)
    left_a = join(1, after(keep_a, right_b), got_a, square1)
    right_a = join(0, after(keep_a, left_a), got_a, square1, far_a)
    left_b = join(1, after(keep_b, right_a), got_b, far_b)
    right_b, left_a = lax.ppermute(right_b, "x", up), lax.ppermute(left_a, "x", down)
    right_a, left_b = lax.ppermute(right_a, "x", up), lax.ppermute(left_b, "x", down)
    return finish(2 * chips, square1, keep_a, keep_b, got_a, got_b, right_a, left_a, right_b, left_b)


def solution(mesh):
    torus = Mesh(mesh.devices.reshape(8, 4, 4, 2), ("z", "y", "x", "c"))
    seq, mp = ("z", "y"), ("x", "c")
    in_specs = (
        P(seq, mp),
        P(seq, mp),
        P(seq, None),
        P(seq, None),
        P(seq, mp),
        P(seq, mp),
        P(mp),
        P(mp),
        P(mp, None),
    )

    return jax.shard_map(body, mesh=torus, in_specs=in_specs, out_specs=P(seq + mp, None), check_vma=False)
```

```python
import functools

import jax
import jax.numpy as jnp
from jax import lax
from jax.experimental import pallas as pl
from jax.experimental.pallas import tpu as pltpu
from jax.sharding import Mesh
from jax.sharding import PartitionSpec as P


BLOCK = 256
HALF = 128
HEADS = 10
WIDTH = 64
CH = HEADS * WIDTH
STATE = 128
ROWS = 1024
NBLK = ROWS // BLOCK
SEQ_DEV = 32
PIECE = STATE // SEQ_DEV
D = 2560
WA = 1408
WB = D - WA
CHUNKS = 8
TILES = WA // HALF * (HALF // 8) + 1
PADH = 16
TALL = HALF + 8
LOG2E = 1.4426950408889634
F32 = jnp.float32
BF16 = jnp.bfloat16


def parts(value, count):
    out = []
    for _ in range(count):
        piece = value.astype(BF16)
        out.append(piece)
        value = value - piece.astype(F32)
    return out


def spread_matrix(count, tail):
    cols = CH + (HALF if tail else 0)
    row = lax.broadcasted_iota(jnp.int32, (PADH * count, cols), 0) % PADH
    col = lax.broadcasted_iota(jnp.int32, (PADH * count, cols), 1)
    head = jnp.where(col < CH, col // WIDTH, col - CH)
    return jnp.where(row == head, 1.0, 0.0).astype(BF16)


def spread(value, matrix, count):
    stacked = jnp.concatenate(parts(value, count), axis=0)
    return lax.dot_general(stacked, matrix, (((0,), (0,)), ((), ())), preferred_element_type=F32)


def triangle():
    row = lax.broadcasted_iota(jnp.int32, (BLOCK, BLOCK), 0)
    return jnp.where(row <= lax.broadcasted_iota(jnp.int32, (BLOCK, BLOCK), 1), 1.0, 0.0).astype(BF16)


def running_sums(value):
    rows = value.shape[0]
    sums = jnp.dot(jnp.concatenate(parts(value, 3), axis=0), triangle(), preferred_element_type=F32)
    return sums[0:rows] + sums[rows : 2 * rows] + sums[2 * rows : 3 * rows]


def state_kernel(
    x_hbm, b_hbm, dt_hbm, ld_hbm, msg_ref, pad_ref, dtp_ref, run_ref, x_ref, b_ref, dt_ref, ld_ref, sem
):
    copies = [pltpu.make_async_copy(ld_hbm, ld_ref, sem.at[0]), pltpu.make_async_copy(dt_hbm, dt_ref, sem.at[1])]
    for k in range(NBLK):
        rows = pl.ds(BLOCK * k, BLOCK)
        copies.append(pltpu.make_async_copy(x_hbm.at[rows, :], x_ref.at[rows, :], sem.at[2 + 2 * k]))
        copies.append(pltpu.make_async_copy(b_hbm.at[rows, :], b_ref.at[rows, :], sem.at[3 + 2 * k]))
    for copy in copies:
        copy.start()
    pad_ref[...] = jnp.zeros_like(pad_ref)
    dtp_ref[...] = jnp.zeros_like(dtp_ref)
    copies[0].wait()
    for k in range(NBLK):
        pad_ref[PADH * k : PADH * k + HEADS, :] = ld_ref[:, BLOCK * k : BLOCK * (k + 1)]
    levels = running_sums(pad_ref[...])
    closings = [levels[PADH * k : PADH * (k + 1), BLOCK - 1 : BLOCK] for k in range(NBLK)]
    tails = [jnp.zeros((PADH, 1), F32)]
    for k in reversed(range(NBLK)):
        tails.insert(0, tails[0] + closings[k])
    lane = lax.broadcasted_iota(jnp.int32, (PADH, HALF), 1)
    decay = spread(jnp.where(lane == 0, tails[0], 0.0), spread_matrix(3, True)[:, CH:], 3)[0:1, :]
    decays = jnp.concatenate([v.astype(F32) for v in parts(decay, 3)] + [jnp.zeros((1, HALF), F32)], axis=0)
    decays = decays.astype(BF16)
    two = spread_matrix(2, False)
    copies[1].wait()
    dtp_ref[0:HEADS, :] = dt_ref[...]
    total = None
    for k in range(NBLK):
        weight = jnp.exp(tails[k] - levels[PADH * k : PADH * (k + 1)]) * dtp_ref[:, BLOCK * k : BLOCK * (k + 1)]
        wide = spread(weight, two, 2)
        copies[2 + 2 * k].wait()
        copies[3 + 2 * k].wait()
        weighted = (wide * x_ref[BLOCK * k : BLOCK * (k + 1), :].astype(F32)).astype(BF16)
        own = lax.dot_general(
            b_ref[BLOCK * k : BLOCK * (k + 1), :], weighted, (((0,), (0,)), ((), ())), preferred_element_type=F32
        )
        total = own if total is None else total + own
    run_ref[...] = total
    for q in range(SEQ_DEV):
        msg_ref[q, :, 0:CH] = run_ref[PIECE * q : PIECE * (q + 1), :].astype(BF16)
        msg_ref[q, :, CH : CH + HALF] = decays


def prefix_kernel(msg_ref, out_hbm, dec_ref, out_ref, sem):
    for i in range(SEQ_DEV):
        for part in range(3):
            dec_ref[part, i : i + 1, :] = msg_ref[i, :, CH : CH + HALF].astype(F32)[part : part + 1]
    head = lax.broadcasted_iota(jnp.int32, (HALF, CH), 0)
    col = lax.broadcasted_iota(jnp.int32, (HALF, CH), 1)
    matrix = jnp.where(head == col // WIDTH, 1.0, 0.0).astype(BF16)
    logs = jnp.zeros((SEQ_DEV, CH), F32)
    for part in range(3):
        logs = logs + jnp.dot(dec_ref[part].astype(BF16), matrix, preferred_element_type=F32)
    decay = jnp.exp(logs)
    running = jnp.zeros((PIECE, CH), F32)
    group = SEQ_DEV // CHUNKS
    copies = []
    for i in range(SEQ_DEV):
        out_ref[i] = running.astype(BF16)
        running = decay[i : i + 1, :] * running + msg_ref[i, :, 0:CH].astype(F32)
        if i % group == group - 1:
            span = pl.ds(i + 1 - group, group)
            copies.append(pltpu.make_async_copy(out_ref.at[span], out_hbm.at[span], sem.at[i // group]))
            copies[-1].start()
    for copy in copies:
        copy.wait()


def local_kernel(
    idx_ref, x_ref, g_ref, b_ref, c_ref, dt_ref, ld_ref, skip_ref, w_hbm, far_gl_ref, far_fs_ref, left_gl_ref, left_fs_ref,
    right_gl_ref, right_fs_ref, own_gl_ref, own_fs_ref, w_ref,
    gl_ref, fs_ref, run_ref, lead_ref, pad_ref, dtp_ref, sem
):
    k = pl.program_id(0)
    fetch = pltpu.make_async_copy(w_hbm.at[:, pl.ds(0, WA)], w_ref, sem.at[0])

    @pl.when(k == 0)
    def _():
        fetch.start()
        run_ref[...] = jnp.zeros_like(run_ref)
        lead_ref[...] = jnp.zeros_like(lead_ref)
        pad_ref[...] = jnp.zeros_like(pad_ref)
        dtp_ref[...] = jnp.zeros_like(dtp_ref)

    pad_ref[0:HEADS, :] = ld_ref[...]
    dtp_ref[0:HEADS, :] = dt_ref[...]
    lev = running_sums(pad_ref[...])
    closing = lev[:, BLOCK - 1 : BLOCK]
    reader, writer = c_ref[...], b_ref[...]
    two = spread_matrix(2, False)
    lane = lax.broadcasted_iota(jnp.int32, (PADH, HALF), 1)
    table = jnp.where(lane == 0, jnp.exp(lead_ref[...]), jnp.where(lane == 1, jnp.exp(closing), 0.0))
    table = spread(table, spread_matrix(3, False), 3)
    lead = table[0:1, :]
    lead_ref[...] += closing
    grown = spread(jnp.exp(lev), two, 2)
    carry = jnp.dot(reader, run_ref[...].astype(BF16), preferred_element_type=F32)
    weight = spread(jnp.exp(closing - lev) * dtp_ref[...], two, 2)
    weighted = (weight * x_ref[...].astype(F32)).astype(BF16)
    own = lax.dot_general(writer, weighted, (((0,), (0,)), ((), ())), preferred_element_type=F32)
    run_ref[...] = table[1:2, :] * run_ref[...] + own
    lev2 = lev * LOG2E
    cols = jnp.transpose(lev2)
    rows = lev2[0:HEADS] - jnp.log(dt_ref[...]) * LOG2E
    inter = lax.dot_general(reader, writer, (((1,), (1,)), ((), ())), preferred_element_type=F32)
    causal = lax.broadcasted_iota(jnp.int32, (HALF, HALF), 0) >= lax.broadcasted_iota(jnp.int32, (HALF, HALF), 1)
    lane = lax.broadcasted_iota(jnp.int32, (HALF, HALF), 1) < WIDTH

    def score(head, r, s):
        gap = cols[HALF * r : HALF * (r + 1), head : head + 1] - rows[head : head + 1, HALF * s : HALF * (s + 1)]
        value = jnp.exp2(gap) * inter[HALF * r : HALF * (r + 1), HALF * s : HALF * (s + 1)]
        if r == s:
            value = jnp.where(causal, value, 0.0)
        return value.astype(BF16)

    for pair in range(HEADS // 2):
        lanes = slice(HALF * pair, HALF * (pair + 1))
        top_x = x_ref[0:HALF, lanes]
        low_x = x_ref[HALF:BLOCK, lanes]
        tops, lows = [], []
        for head in (2 * pair, 2 * pair + 1):
            tops.append(jnp.dot(score(head, 0, 0), top_x, preferred_element_type=F32))
            lows.append(
                jnp.dot(score(head, 1, 0), top_x, preferred_element_type=F32)
                + jnp.dot(score(head, 1, 1), low_x, preferred_element_type=F32)
            )
        for r, (even, odd), x_part in ((0, tops, top_x), (1, lows, low_x)):
            span = slice(HALF * r, HALF * (r + 1))
            mixed = (
                jnp.where(lane, even, odd)
                + grown[span, lanes] * carry[span, lanes]
                + skip_ref[:, lanes] * x_part.astype(F32)
            )
            gate = g_ref[span, lanes].astype(F32)
            gate = gate / (1.0 + jnp.exp(-gate))
            gl_ref[span, lanes] = (mixed * gate).astype(BF16)
            fs_ref[span, lanes] = (grown[span, lanes] * lead[:, lanes] * gate).astype(BF16)

    roles = (
        (far_gl_ref, far_fs_ref),
        (left_gl_ref, left_fs_ref),
        (right_gl_ref, right_fs_ref),
        (own_gl_ref, own_fs_ref),
    )
    for role, (to_gl_ref, to_fs_ref) in enumerate(roles):

        @pl.when(k == idx_ref[1 + role])
        def _():
            to_gl_ref[...] = gl_ref[...]
            to_fs_ref[...] = fs_ref[...]

    @pl.when(k == NBLK - 1)
    def _():
        fetch.wait()


def square_rows(total):
    rows = [piece.astype(F32) for piece in parts(total, 3)]
    return jnp.concatenate(rows + [jnp.zeros((8 - len(rows), HALF), F32)], axis=0).astype(BF16)


def squares_of(ref, first):
    return jnp.sum(ref[first : first + 8, 0:HALF].astype(F32), axis=0, keepdims=True)


def gate_block(place, idx_ref, state, gain, c_ref, gl_ref, fs_ref, rows_ref, square_ref):
    squares = []
    for n, half in enumerate((1 - idx_ref[0], idx_ref[0])):
        there = pl.ds(pl.multiple_of((2 * idx_ref[place] + half) * HALF, HALF), HALF)
        here = pl.ds(pl.multiple_of(half * HALF, HALF), HALF)
        gated = gl_ref[here, :].astype(F32) + fs_ref[here, :].astype(F32) * jnp.dot(
            c_ref[there, :], state, preferred_element_type=F32
        )
        sums = jnp.sum(gated * gated, axis=1, keepdims=True)
        squares.append(jnp.transpose(jnp.broadcast_to(sums, (HALF, HALF)))[0:1, :])
        rows_ref[HALF * n : HALF * (n + 1), :] = (gated * gain).astype(BF16)
    square_ref[...] = jnp.concatenate(squares + [jnp.zeros((8 - len(squares), HALF), F32)], axis=0)


def gate_kernel(place, idx_ref, p_ref, gain_ref, c_ref, gl_ref, fs_ref, rows_ref, square_ref, *rest):
    if rest:
        p_out_ref, st_ref = rest
        for q in range(SEQ_DEV):
            st_ref[PIECE * q : PIECE * (q + 1), :] = p_ref[q].astype(F32)
        state = st_ref[...].astype(BF16)
        p_out_ref[...] = state
    else:
        state = p_ref[...]
    gate_block(place, idx_ref, state, gain_ref[...], c_ref, gl_ref, fs_ref, rows_ref, square_ref)


def product_kernel(rows_ref, square_ref, w_ref, send_ref, keep_ref):
    width = keep_ref.shape[1]
    rows = rows_ref[...]
    for base in range(0, width, BLOCK):
        cols = slice(base, min(base + BLOCK, width))
        value = jnp.dot(rows, w_ref[:, cols], preferred_element_type=F32)
        keep_ref[:, cols] = value[HALF:BLOCK]
        send_ref[0:HALF, cols] = value[0:HALF].astype(BF16)
    if send_ref.shape[0] == TALL:
        send_ref[HALF:TALL, 0:HALF] = square_rows(square_ref[0:1, :])
        send_ref[HALF:TALL, HALF:width] = jnp.zeros((TALL - HALF, width - HALF), BF16)


def middle_kernel(
    idx_ref, p_ref, gain_ref, c_ref, left_gl_ref, left_fs_ref, far_rows_ref, far_square_ref, right_gl_hbm, right_fs_hbm, w_hbm,
    send_ref, keep_ref, left_rows_ref, left_square_ref, right_rows_ref, right_square_ref, w_ref,
    right_gl_ref, right_fs_ref, sem
):
    fetches = [
        pltpu.make_async_copy(right_gl_hbm, right_gl_ref, sem.at[0]),
        pltpu.make_async_copy(right_fs_hbm, right_fs_ref, sem.at[1]),
        pltpu.make_async_copy(w_hbm.at[:, pl.ds(WA, WB)], w_ref, sem.at[2]),
    ]
    for fetch in fetches:
        fetch.start()
    state, gain = p_ref[...], gain_ref[...]
    gate_block(2, idx_ref, state, gain, c_ref, left_gl_ref, left_fs_ref, left_rows_ref, left_square_ref)
    fetches[0].wait()
    fetches[1].wait()
    gate_block(3, idx_ref, state, gain, c_ref, right_gl_ref, right_fs_ref, right_rows_ref, right_square_ref)
    fetches[2].wait()
    product_kernel(far_rows_ref, far_square_ref, w_ref, send_ref, keep_ref)


def tiles_of(width):
    per_row = width // HALF
    for n in range(HALF // 8 * per_row):
        yield n, n // per_row * 8, slice(n % per_row * HALF, (n % per_row + 1) * HALF)


def join_kernel(keep_ref, got_ref, *refs):
    out_ref = refs[-1]
    if got_ref.shape[0] == HALF:
        value = keep_ref[...] + got_ref[...].astype(F32)
        for ref in refs[:-1]:
            value = value + ref[...].astype(F32)
        out_ref[...] = value.astype(BF16)
        return
    square_ref, more = refs[0], refs[1:-1]
    for n, row, lanes in tiles_of(keep_ref.shape[1]):
        value = keep_ref[row : row + 8, lanes] + got_ref[row : row + 8, lanes].astype(F32)
        for ref in more:
            value = value + ref[n].astype(F32)
        out_ref[n] = value.astype(BF16)
    total = square_ref[1:2, :] + squares_of(got_ref, HALF)
    for ref in more:
        total = total + last_squares(ref)
    out_ref[TILES - 1] = square_rows(total)


def last_squares(ref):
    return jnp.sum(ref[TILES - 1].astype(F32), axis=0, keepdims=True)


def finish_kernel(
    devices, square_ref, ka_ref, kb_ref, ga_ref, gb_ref, ra_ref, la_ref, rb_ref, lb_ref, out_hbm, scale_ref, out_ref, sem
):
    total = square_ref[1:2, :] + squares_of(ga_ref, HALF) + last_squares(ra_ref) + last_squares(la_ref)
    scale = lax.rsqrt(total / (CH * devices) + 1e-05)
    scale_ref[...] = jnp.transpose(jnp.broadcast_to(scale, (HALF, HALF)))
    copies = []
    group = HALF // CHUNKS
    for n, row, lanes in tiles_of(WA):
        span = slice(row, row + 8)
        value = ka_ref[span, lanes] + ga_ref[span, lanes].astype(F32) + ra_ref[n].astype(F32) + la_ref[n].astype(F32)
        out_ref[span, lanes] = (value * scale_ref[span, 0:1]).astype(BF16)
        if lanes.stop == WA and (row + 8) % group == 0:
            span = slice(row + 8 - group, row + 8)
            value = kb_ref[span, :] + gb_ref[span, :].astype(F32) + rb_ref[span, :].astype(F32)
            value = value + lb_ref[span, :].astype(F32)
            out_ref[span, WA:D] = (value * scale_ref[span, 0:1]).astype(BF16)
            span = pl.ds(row + 8 - group, group)
            copies.append(pltpu.make_async_copy(out_ref.at[span, :], out_hbm.at[span, :], sem.at[len(copies)]))
            copies[-1].start()
    for copy in copies:
        copy.wait()


VMEM = pl.BlockSpec(memory_space=pltpu.VMEM)
SMEM = pl.BlockSpec(memory_space=pltpu.SMEM)
HBM = pl.BlockSpec(memory_space=pltpu.HBM)
LIMIT = 24 * 1024 * 1024


def local_call(kernel, args, outs, scratch=(), flops=1e8, in_specs=None, out_specs=None):
    in_specs, out_specs = in_specs or [VMEM] * len(args), out_specs or [VMEM] * len(outs)
    args = [pltpu.with_memory_space_constraint(v, pltpu.HBM) if spec is HBM else v for v, spec in zip(args, in_specs)]
    return pl.pallas_call(
        kernel,
        in_specs=in_specs,
        out_specs=out_specs,
        out_shape=[
            pltpu.HBM(*out) if spec is HBM else jax.ShapeDtypeStruct(*out) for out, spec in zip(outs, out_specs)
        ],
        scratch_shapes=[pltpu.VMEM(*v) if isinstance(v, tuple) else pltpu.SemaphoreType.DMA((v,)) for v in scratch],
        cost_estimate=pl.CostEstimate(flops=int(flops), bytes_accessed=0, transcendentals=0),
        compiler_params=pltpu.CompilerParams(vmem_limit_bytes=LIMIT),
    )(*args)


def local_state(x, b, dt, ld):
    outs = (((SEQ_DEV, PIECE, CH + HALF), BF16),)
    scratch = [
        ((PADH * NBLK, BLOCK), F32),
        ((PADH, ROWS), F32),
        ((STATE, CH), F32),
        ((ROWS, CH), BF16),
        ((ROWS, STATE), BF16),
        ((HEADS, ROWS), F32),
        ((HEADS, ROWS), F32),
        2 + 2 * NBLK,
    ]
    return local_call(state_kernel, (x, b, dt, ld), outs, scratch, 1e9, [HBM] * 4)[0]


def seq_prefix(msg):
    outs = (((SEQ_DEV, PIECE, CH), BF16),)
    scratch = [((3, SEQ_DEV, HALF), F32), outs[0], CHUNKS]
    return local_call(prefix_kernel, (msg,), outs, scratch, out_specs=[HBM])[0]


def whole(shape):
    return pl.BlockSpec(shape, lambda *_: (0,) * len(shape))


def local_part(order, x, g, b, c, dt, ld, skip, w):
    rows = lambda width: pl.BlockSpec((BLOCK, width), lambda k: (k, 0))
    heads = pl.BlockSpec((HEADS, BLOCK), lambda k: (0, k))
    there = lambda v: pltpu.with_memory_space_constraint(v, pltpu.HBM)
    return pl.pallas_call(
        local_kernel,
        grid=(NBLK,),
        in_specs=[SMEM, rows(CH), rows(CH), rows(STATE), rows(STATE), heads, heads, whole((1, CH)), HBM],
        out_specs=(VMEM,) * 4 + (whole((BLOCK, CH)),) * 4 + (VMEM,),
        out_shape=(jax.ShapeDtypeStruct((BLOCK, CH), BF16),) * 4
        + (pltpu.HBM((BLOCK, CH), BF16),) * 4
        + (jax.ShapeDtypeStruct((CH, WA), BF16),),
        scratch_shapes=[
            pltpu.VMEM((BLOCK, CH), BF16),
            pltpu.VMEM((BLOCK, CH), BF16),
            pltpu.VMEM((STATE, CH), F32),
            pltpu.VMEM((PADH, HALF), F32),
            pltpu.VMEM((PADH, BLOCK), F32),
            pltpu.VMEM((PADH, BLOCK), F32),
            pltpu.SemaphoreType.DMA((1,)),
        ],
        cost_estimate=pl.CostEstimate(flops=int(3e9), bytes_accessed=0, transcendentals=0),
        compiler_params=pltpu.CompilerParams(vmem_limit_bytes=LIMIT),
        name="local_part",
    )(order, *(there(v) for v in (x, g, b, c, dt, ld)), skip, there(w))


def gated_rows(order, place, prefix, *args):
    outs = [((BLOCK, CH), BF16), ((8, HALF), F32)]
    scratch = []
    if prefix.ndim == 3:
        outs.append(((STATE, CH), BF16))
        scratch.append(((STATE, CH), F32))
    kernel = functools.partial(gate_kernel, place)
    return local_call(kernel, (order, prefix, *args), outs, scratch, 5e8, [SMEM] + [VMEM] * 5)


def product(rows, squares, w):
    width = w.shape[1]
    tall = TALL if width == WA else HALF
    outs = [((tall, width), BF16), ((HALF, width), F32)]
    return local_call(product_kernel, (rows, squares, w), outs, (), 2 * BLOCK * CH * width)


def middle(*args):
    gated = [((BLOCK, CH), BF16), ((8, HALF), F32)]
    outs = [((HALF, WB), BF16), ((HALF, WB), F32), *gated, *gated, ((CH, WB), BF16)]
    scratch = [gated[0], gated[0], 3]
    in_specs = [SMEM] + [VMEM] * 7 + [HBM] * 3
    return local_call(middle_kernel, args, outs, scratch, 2e9, in_specs)


def join(keep, got, *more):
    out = (TILES, 8, HALF) if got.shape[0] == TALL else keep.shape
    return local_call(join_kernel, (keep, got, *more), ((out, BF16),))[0]


def finish(devices, *args):
    kernel = functools.partial(finish_kernel, devices)
    out = ((HALF, D), BF16)
    scratch = [((HALF, HALF), F32), out, CHUNKS]
    return local_call(kernel, args, (out,), scratch, out_specs=[HBM])[0]


def after(value, earlier):
    return lax.optimization_barrier((value, earlier))[0]


def body(x, g, b, c, dt, ld, skip, gain, w):
    chips = lax.axis_size("x")
    chip, core = lax.axis_index("x"), lax.axis_index("c")
    up = [(i, (i + 1) % chips) for i in range(chips)]
    down = [(i, (i - 1) % chips) for i in range(chips)]
    swap = [(0, 1), (1, 0)]
    order = jnp.stack([core, (chip + 2) % chips, (chip + 3) % chips, (chip + 1) % chips, chip]).astype(jnp.int32)
    msg = local_state(x, b, dt.T, ld.T)
    msg = lax.all_to_all(msg, ("z", "y"), split_axis=0, concat_axis=0, tiled=True)
    skip_wide = jnp.repeat(skip, WIDTH)[None, :]
    *parts_of, w_a = local_part(order, x, g, b, c, dt.T, ld.T, skip_wide, w)
    far, left, right, own = (parts_of[2 * i : 2 * i + 2] for i in range(4))
    prefix = lax.all_to_all(seq_prefix(msg), ("z", "y"), split_axis=0, concat_axis=0, tiled=True)
    gain_row = gain.astype(F32)[None, :]

    rows, square, prefix = gated_rows(order, 1, prefix, gain_row, c, *far)
    send, far_keep_a = product(rows, square, w_a)
    far_got_a = lax.ppermute(send, "c", swap)
    send, far_keep_b, rows_left, square_left, rows_right, square_right, w_b = middle(
        order, prefix, gain_row, c, *left, after(rows, send), square, *right, w
    )
    far_got_b = lax.ppermute(send, "c", swap)
    far_a = join(after(far_keep_a, send), far_got_a, square)
    last = far_b = join(after(far_keep_b, far_a), far_got_b)
    far_a, far_b = lax.ppermute(far_a, "x", up), lax.ppermute(far_b, "x", down)

    send, left_keep_a = product(after(rows_left, last), square_left, w_a)
    left_got_a = lax.ppermute(send, "c", swap)
    send, right_keep_b = product(after(rows_right, send), square_right, w_b)
    right_got_b = lax.ppermute(send, "c", swap)
    last = left_a = join(after(left_keep_a, send), left_got_a, square_left)
    left_a = lax.ppermute(left_a, "x", down)
    last = right_b = join(after(right_keep_b, last), right_got_b)
    right_b = lax.ppermute(right_b, "x", up)
    send, right_keep_a = product(after(rows_right, last), square_right, w_a)
    right_got_a = lax.ppermute(send, "c", swap)
    send, left_keep_b = product(after(rows_left, send), square_left, w_b)
    left_got_b = lax.ppermute(send, "c", swap)
    last = right_a = join(after(right_keep_a, send), right_got_a, square_right, far_a)
    right_a = lax.ppermute(right_a, "x", up)
    last = left_b = join(after(left_keep_b, last), left_got_b, far_b)
    left_b = lax.ppermute(left_b, "x", down)

    rows, square = gated_rows(order, 4, after(prefix, last), gain_row, c, *own)
    send, keep_a = product(rows, square, w_a)
    got_a = lax.ppermute(send, "c", swap)
    send, keep_b = product(after(rows, send), square, w_b)
    got_b = lax.ppermute(send, "c", swap)
    return finish(2 * chips, square, keep_a, keep_b, got_a, got_b, right_a, left_a, right_b, left_b)


def solution(mesh):
    torus = Mesh(mesh.devices.reshape(8, 4, 4, 2), ("z", "y", "x", "c"))
    seq, mp = ("z", "y"), ("x", "c")
    in_specs = (
        P(seq, mp),
        P(seq, mp),
        P(seq, None),
        P(seq, None),
        P(seq, mp),
        P(seq, mp),
        P(mp),
        P(mp),
        P(mp, None),
    )

    return jax.shard_map(body, mesh=torus, in_specs=in_specs, out_specs=P(seq + mp, None), check_vma=False)
```

```python
import functools

import jax
import jax.numpy as jnp
from jax import lax
from jax.experimental import pallas as pl
from jax.experimental.pallas import tpu as pltpu
from jax.sharding import Mesh
from jax.sharding import PartitionSpec as P


BLOCK = 256
HALF = 128
HEADS = 10
WIDTH = 64
CH = HEADS * WIDTH
STATE = 128
ROWS = 1024
NBLK = ROWS // BLOCK
SEQ_DEV = 32
PIECE = STATE // SEQ_DEV
D = 2560
WA = 1408
WB = D - WA
CHUNKS = 8
TILES = WA // HALF * (HALF // 8) + 1
PADH = 16
TALL = HALF + 8
LOG2E = 1.4426950408889634
F32 = jnp.float32
BF16 = jnp.bfloat16


def parts(value, count):
    out = []
    for _ in range(count):
        piece = value.astype(BF16)
        out.append(piece)
        value = value - piece.astype(F32)
    return out


def spread_matrix(count, tail):
    cols = CH + (HALF if tail else 0)
    row = lax.broadcasted_iota(jnp.int32, (PADH * count, cols), 0) % PADH
    col = lax.broadcasted_iota(jnp.int32, (PADH * count, cols), 1)
    head = jnp.where(col < CH, col // WIDTH, col - CH)
    return jnp.where(row == head, 1.0, 0.0).astype(BF16)


def spread(value, matrix, count):
    stacked = jnp.concatenate(parts(value, count), axis=0)
    return lax.dot_general(stacked, matrix, (((0,), (0,)), ((), ())), preferred_element_type=F32)


def triangle():
    row = lax.broadcasted_iota(jnp.int32, (BLOCK, BLOCK), 0)
    return jnp.where(row <= lax.broadcasted_iota(jnp.int32, (BLOCK, BLOCK), 1), 1.0, 0.0).astype(BF16)


def running_sums(value, upper):
    rows = value.shape[0]
    sums = jnp.dot(jnp.concatenate(parts(value, 3), axis=0), upper, preferred_element_type=F32)
    return sums[0:rows] + sums[rows : 2 * rows] + sums[2 * rows : 3 * rows]


def state_kernel(
    x_hbm, b_hbm, dt_hbm, ld_hbm, msg_ref, pad_ref, dtp_ref, run_ref, x_ref, b_ref, dt_ref, ld_ref,
    upper_ref, two_ref, sem
):
    copies = [pltpu.make_async_copy(ld_hbm, ld_ref, sem.at[0]), pltpu.make_async_copy(dt_hbm, dt_ref, sem.at[1])]
    for k in range(NBLK):
        rows = pl.ds(BLOCK * k, BLOCK)
        copies.append(pltpu.make_async_copy(x_hbm.at[rows, :], x_ref.at[rows, :], sem.at[2 + 2 * k]))
        copies.append(pltpu.make_async_copy(b_hbm.at[rows, :], b_ref.at[rows, :], sem.at[3 + 2 * k]))
    for copy in copies:
        copy.start()
    pad_ref[...] = jnp.zeros_like(pad_ref)
    dtp_ref[...] = jnp.zeros_like(dtp_ref)
    upper_ref[...] = triangle()
    two_ref[...] = spread_matrix(2, False)
    copies[0].wait()
    for k in range(NBLK):
        pad_ref[PADH * k : PADH * k + HEADS, :] = ld_ref[:, BLOCK * k : BLOCK * (k + 1)]
    levels = running_sums(pad_ref[...], upper_ref[...])
    closings = [levels[PADH * k : PADH * (k + 1), BLOCK - 1 : BLOCK] for k in range(NBLK)]
    tails = [jnp.zeros((PADH, 1), F32)]
    for k in reversed(range(NBLK)):
        tails.insert(0, tails[0] + closings[k])
    lane = lax.broadcasted_iota(jnp.int32, (PADH, HALF), 1)
    decay = spread(jnp.where(lane == 0, tails[0], 0.0), spread_matrix(3, True)[:, CH:], 3)[0:1, :]
    decays = jnp.concatenate([v.astype(F32) for v in parts(decay, 3)] + [jnp.zeros((1, HALF), F32)], axis=0)
    decays = decays.astype(BF16)
    two = two_ref[...]
    copies[1].wait()
    dtp_ref[0:HEADS, :] = dt_ref[...]
    wides = []
    for k in range(NBLK):
        weight = jnp.exp(tails[k] - levels[PADH * k : PADH * (k + 1)]) * dtp_ref[:, BLOCK * k : BLOCK * (k + 1)]
        wides.append(spread(weight, two, 2))
    for copy in copies[2:]:
        copy.wait()
    total = None
    for k in range(NBLK):
        weighted = (wides[k] * x_ref[BLOCK * k : BLOCK * (k + 1), :].astype(F32)).astype(BF16)
        own = lax.dot_general(
            b_ref[BLOCK * k : BLOCK * (k + 1), :], weighted, (((0,), (0,)), ((), ())), preferred_element_type=F32
        )
        total = own if total is None else total + own
    run_ref[...] = total
    for q in range(SEQ_DEV):
        msg_ref[q, :, 0:CH] = run_ref[PIECE * q : PIECE * (q + 1), :].astype(BF16)
        msg_ref[q, :, CH : CH + HALF] = decays


def prefix_kernel(msg_ref, out_hbm, dec_ref, out_ref, sem):
    for i in range(SEQ_DEV):
        for part in range(3):
            dec_ref[part, i : i + 1, :] = msg_ref[i, :, CH : CH + HALF].astype(F32)[part : part + 1]
    head = lax.broadcasted_iota(jnp.int32, (HALF, CH), 0)
    col = lax.broadcasted_iota(jnp.int32, (HALF, CH), 1)
    matrix = jnp.where(head == col // WIDTH, 1.0, 0.0).astype(BF16)
    logs = jnp.zeros((SEQ_DEV, CH), F32)
    for part in range(3):
        logs = logs + jnp.dot(dec_ref[part].astype(BF16), matrix, preferred_element_type=F32)
    decay = jnp.exp(logs)
    running = jnp.zeros((PIECE, CH), F32)
    group = SEQ_DEV // CHUNKS
    copies = []
    for i in range(SEQ_DEV):
        out_ref[i] = running.astype(BF16)
        running = decay[i : i + 1, :] * running + msg_ref[i, :, 0:CH].astype(F32)
        if i % group == group - 1:
            span = pl.ds(i + 1 - group, group)
            copies.append(pltpu.make_async_copy(out_ref.at[span], out_hbm.at[span], sem.at[i // group]))
            copies[-1].start()
    for copy in copies:
        copy.wait()


def local_kernel(
    idx_ref, x_ref, g_ref, b_ref, c_ref, dt_ref, ld_ref, skip_ref, w_hbm, far_gl_ref, far_fs_ref, left_gl_ref, left_fs_ref,
    right_gl_ref, right_fs_ref, own_gl_ref, own_fs_ref, w_ref,
    gl_ref, fs_ref, run_ref, lead_ref, pad_ref, dtp_ref, sem
):
    k = pl.program_id(0)
    fetch = pltpu.make_async_copy(w_hbm.at[:, pl.ds(0, WA)], w_ref, sem.at[0])

    @pl.when(k == 0)
    def _():
        fetch.start()
        run_ref[...] = jnp.zeros_like(run_ref)
        lead_ref[...] = jnp.zeros_like(lead_ref)
        pad_ref[...] = jnp.zeros_like(pad_ref)
        dtp_ref[...] = jnp.zeros_like(dtp_ref)

    pad_ref[0:HEADS, :] = ld_ref[...]
    dtp_ref[0:HEADS, :] = dt_ref[...]
    lev = running_sums(pad_ref[...], triangle())
    closing = lev[:, BLOCK - 1 : BLOCK]
    reader, writer = c_ref[...], b_ref[...]
    two = spread_matrix(2, False)
    lane = lax.broadcasted_iota(jnp.int32, (PADH, HALF), 1)
    table = jnp.where(lane == 0, jnp.exp(lead_ref[...]), jnp.where(lane == 1, jnp.exp(closing), 0.0))
    table = spread(table, spread_matrix(3, False), 3)
    lead = table[0:1, :]
    lead_ref[...] += closing
    grown = spread(jnp.exp(lev), two, 2)
    carry = jnp.dot(reader, run_ref[...].astype(BF16), preferred_element_type=F32)
    weight = spread(jnp.exp(closing - lev) * dtp_ref[...], two, 2)
    weighted = (weight * x_ref[...].astype(F32)).astype(BF16)
    own = lax.dot_general(writer, weighted, (((0,), (0,)), ((), ())), preferred_element_type=F32)
    run_ref[...] = table[1:2, :] * run_ref[...] + own
    lev2 = lev * LOG2E
    cols = jnp.transpose(lev2)
    rows = lev2[0:HEADS] - jnp.log(dt_ref[...]) * LOG2E
    inter = lax.dot_general(reader, writer, (((1,), (1,)), ((), ())), preferred_element_type=F32)
    causal = lax.broadcasted_iota(jnp.int32, (HALF, HALF), 0) >= lax.broadcasted_iota(jnp.int32, (HALF, HALF), 1)
    lane = lax.broadcasted_iota(jnp.int32, (HALF, HALF), 1) < WIDTH

    def score(head, r, s):
        gap = cols[HALF * r : HALF * (r + 1), head : head + 1] - rows[head : head + 1, HALF * s : HALF * (s + 1)]
        value = jnp.exp2(gap) * inter[HALF * r : HALF * (r + 1), HALF * s : HALF * (s + 1)]
        if r == s:
            value = jnp.where(causal, value, 0.0)
        return value.astype(BF16)

    for pair in range(HEADS // 2):
        lanes = slice(HALF * pair, HALF * (pair + 1))
        top_x = x_ref[0:HALF, lanes]
        low_x = x_ref[HALF:BLOCK, lanes]
        tops, lows = [], []
        for head in (2 * pair, 2 * pair + 1):
            tops.append(jnp.dot(score(head, 0, 0), top_x, preferred_element_type=F32))
            lows.append(
                jnp.dot(score(head, 1, 0), top_x, preferred_element_type=F32)
                + jnp.dot(score(head, 1, 1), low_x, preferred_element_type=F32)
            )
        for r, (even, odd), x_part in ((0, tops, top_x), (1, lows, low_x)):
            span = slice(HALF * r, HALF * (r + 1))
            mixed = (
                jnp.where(lane, even, odd)
                + grown[span, lanes] * carry[span, lanes]
                + skip_ref[:, lanes] * x_part.astype(F32)
            )
            gate = g_ref[span, lanes].astype(F32)
            gate = gate / (1.0 + jnp.exp(-gate))
            gl_ref[span, lanes] = (mixed * gate).astype(BF16)
            fs_ref[span, lanes] = (grown[span, lanes] * lead[:, lanes] * gate).astype(BF16)

    roles = (
        (far_gl_ref, far_fs_ref),
        (left_gl_ref, left_fs_ref),
        (right_gl_ref, right_fs_ref),
        (own_gl_ref, own_fs_ref),
    )
    for role, (to_gl_ref, to_fs_ref) in enumerate(roles):

        @pl.when(k == idx_ref[1 + role])
        def _():
            to_gl_ref[...] = gl_ref[...]
            to_fs_ref[...] = fs_ref[...]

    @pl.when(k == NBLK - 1)
    def _():
        fetch.wait()


def square_rows(total):
    rows = [piece.astype(F32) for piece in parts(total, 3)]
    return jnp.concatenate(rows + [jnp.zeros((8 - len(rows), HALF), F32)], axis=0).astype(BF16)


def squares_of(ref, first):
    return jnp.sum(ref[first : first + 8, 0:HALF].astype(F32), axis=0, keepdims=True)


def gate_block(place, idx_ref, state, gain, c_ref, gl_ref, fs_ref, rows_ref, square_ref):
    squares = []
    for n, half in enumerate((1 - idx_ref[0], idx_ref[0])):
        there = pl.ds(pl.multiple_of((2 * idx_ref[place] + half) * HALF, HALF), HALF)
        here = pl.ds(pl.multiple_of(half * HALF, HALF), HALF)
        gated = gl_ref[here, :].astype(F32) + fs_ref[here, :].astype(F32) * jnp.dot(
            c_ref[there, :], state, preferred_element_type=F32
        )
        sums = jnp.sum(gated * gated, axis=1, keepdims=True)
        squares.append(jnp.transpose(jnp.broadcast_to(sums, (HALF, HALF)))[0:1, :])
        rows_ref[HALF * n : HALF * (n + 1), :] = (gated * gain).astype(BF16)
    square_ref[...] = jnp.concatenate(squares + [jnp.zeros((8 - len(squares), HALF), F32)], axis=0)


def gate_kernel(place, idx_ref, p_ref, gain_ref, c_ref, gl_ref, fs_ref, rows_ref, square_ref, *rest):
    if rest:
        p_out_ref, st_ref = rest
        for q in range(SEQ_DEV):
            st_ref[PIECE * q : PIECE * (q + 1), :] = p_ref[q].astype(F32)
        state = st_ref[...].astype(BF16)
        p_out_ref[...] = state
    else:
        state = p_ref[...]
    gate_block(place, idx_ref, state, gain_ref[...], c_ref, gl_ref, fs_ref, rows_ref, square_ref)


def product_kernel(rows_ref, square_ref, w_ref, send_ref, keep_ref):
    width = keep_ref.shape[1]
    rows = rows_ref[...]
    for base in range(0, width, BLOCK):
        cols = slice(base, min(base + BLOCK, width))
        value = jnp.dot(rows, w_ref[:, cols], preferred_element_type=F32)
        keep_ref[:, cols] = value[HALF:BLOCK]
        send_ref[0:HALF, cols] = value[0:HALF].astype(BF16)
    if send_ref.shape[0] == TALL:
        send_ref[HALF:TALL, 0:HALF] = square_rows(square_ref[0:1, :])
        send_ref[HALF:TALL, HALF:width] = jnp.zeros((TALL - HALF, width - HALF), BF16)


def middle_kernel(
    idx_ref, p_ref, gain_ref, c_ref, left_gl_ref, left_fs_ref, far_rows_ref, far_square_ref, right_gl_hbm, right_fs_hbm, w_hbm,
    send_ref, keep_ref, left_rows_ref, left_square_ref, right_rows_ref, right_square_ref, w_ref,
    right_gl_ref, right_fs_ref, sem
):
    fetches = [
        pltpu.make_async_copy(right_gl_hbm, right_gl_ref, sem.at[0]),
        pltpu.make_async_copy(right_fs_hbm, right_fs_ref, sem.at[1]),
        pltpu.make_async_copy(w_hbm.at[:, pl.ds(WA, WB)], w_ref, sem.at[2]),
    ]
    for fetch in fetches:
        fetch.start()
    state, gain = p_ref[...], gain_ref[...]
    gate_block(2, idx_ref, state, gain, c_ref, left_gl_ref, left_fs_ref, left_rows_ref, left_square_ref)
    fetches[0].wait()
    fetches[1].wait()
    gate_block(3, idx_ref, state, gain, c_ref, right_gl_ref, right_fs_ref, right_rows_ref, right_square_ref)
    fetches[2].wait()
    product_kernel(far_rows_ref, far_square_ref, w_ref, send_ref, keep_ref)


def tiles_of(width):
    per_row = width // HALF
    for n in range(HALF // 8 * per_row):
        yield n, n // per_row * 8, slice(n % per_row * HALF, (n % per_row + 1) * HALF)


def join_kernel(keep_ref, got_ref, *refs):
    out_ref = refs[-1]
    if got_ref.shape[0] == HALF:
        value = keep_ref[...] + got_ref[...].astype(F32)
        for ref in refs[:-1]:
            value = value + ref[...].astype(F32)
        out_ref[...] = value.astype(BF16)
        return
    square_ref, more = refs[0], refs[1:-1]
    for n, row, lanes in tiles_of(keep_ref.shape[1]):
        value = keep_ref[row : row + 8, lanes] + got_ref[row : row + 8, lanes].astype(F32)
        for ref in more:
            value = value + ref[n].astype(F32)
        out_ref[n] = value.astype(BF16)
    total = square_ref[1:2, :] + squares_of(got_ref, HALF)
    for ref in more:
        total = total + last_squares(ref)
    out_ref[TILES - 1] = square_rows(total)


def last_squares(ref):
    return jnp.sum(ref[TILES - 1].astype(F32), axis=0, keepdims=True)


def base_kernel(square_ref, ka_ref, kb_ref, ga_ref, gb_ref, la_ref, rb_ref, base_ref, total_ref):
    total = square_ref[1:2, :] + squares_of(ga_ref, HALF) + last_squares(la_ref)
    total_ref[...] = jnp.broadcast_to(total, total_ref.shape)
    for n, row, lanes in tiles_of(WA):
        span = slice(row, row + 8)
        base_ref[span, lanes] = ka_ref[span, lanes] + ga_ref[span, lanes].astype(F32) + la_ref[n].astype(F32)
    base_ref[:, WA:D] = kb_ref[...] + gb_ref[...].astype(F32) + rb_ref[...].astype(F32)


def finish_kernel(devices, total_ref, base_ref, ra_ref, lb_ref, out_hbm, scale_ref, out_ref, sem):
    total = total_ref[0:1, :] + last_squares(ra_ref)
    scale = lax.rsqrt(total / (CH * devices) + 1e-05)
    scale_ref[...] = jnp.transpose(jnp.broadcast_to(scale, (HALF, HALF)))
    copies = []
    group = HALF // CHUNKS
    for n, row, lanes in tiles_of(WA):
        span = slice(row, row + 8)
        out_ref[span, lanes] = ((base_ref[span, lanes] + ra_ref[n].astype(F32)) * scale_ref[span, 0:1]).astype(BF16)
        if lanes.stop == WA and (row + 8) % group == 0:
            span = slice(row + 8 - group, row + 8)
            value = base_ref[span, WA:D] + lb_ref[span, :].astype(F32)
            out_ref[span, WA:D] = (value * scale_ref[span, 0:1]).astype(BF16)
            span = pl.ds(row + 8 - group, group)
            copies.append(pltpu.make_async_copy(out_ref.at[span, :], out_hbm.at[span, :], sem.at[len(copies)]))
            copies[-1].start()
    for copy in copies:
        copy.wait()


VMEM = pl.BlockSpec(memory_space=pltpu.VMEM)
SMEM = pl.BlockSpec(memory_space=pltpu.SMEM)
HBM = pl.BlockSpec(memory_space=pltpu.HBM)
LIMIT = 24 * 1024 * 1024


def local_call(kernel, args, outs, scratch=(), flops=1e8, in_specs=None, out_specs=None):
    in_specs, out_specs = in_specs or [VMEM] * len(args), out_specs or [VMEM] * len(outs)
    args = [pltpu.with_memory_space_constraint(v, pltpu.HBM) if spec is HBM else v for v, spec in zip(args, in_specs)]
    return pl.pallas_call(
        kernel,
        in_specs=in_specs,
        out_specs=out_specs,
        out_shape=[
            pltpu.HBM(*out) if spec is HBM else jax.ShapeDtypeStruct(*out) for out, spec in zip(outs, out_specs)
        ],
        scratch_shapes=[pltpu.VMEM(*v) if isinstance(v, tuple) else pltpu.SemaphoreType.DMA((v,)) for v in scratch],
        cost_estimate=pl.CostEstimate(flops=int(flops), bytes_accessed=0, transcendentals=0),
        compiler_params=pltpu.CompilerParams(vmem_limit_bytes=LIMIT),
    )(*args)


def local_state(x, b, dt, ld):
    outs = (((SEQ_DEV, PIECE, CH + HALF), BF16),)
    scratch = [
        ((PADH * NBLK, BLOCK), F32),
        ((PADH, ROWS), F32),
        ((STATE, CH), F32),
        ((ROWS, CH), BF16),
        ((ROWS, STATE), BF16),
        ((HEADS, ROWS), F32),
        ((HEADS, ROWS), F32),
        ((BLOCK, BLOCK), BF16),
        ((2 * PADH, CH), BF16),
        2 + 2 * NBLK,
    ]
    return local_call(state_kernel, (x, b, dt, ld), outs, scratch, 1e9, [HBM] * 4)[0]


def seq_prefix(msg):
    outs = (((SEQ_DEV, PIECE, CH), BF16),)
    scratch = [((3, SEQ_DEV, HALF), F32), outs[0], CHUNKS]
    return local_call(prefix_kernel, (msg,), outs, scratch, out_specs=[HBM])[0]


def whole(shape):
    return pl.BlockSpec(shape, lambda *_: (0,) * len(shape))


def local_part(order, x, g, b, c, dt, ld, skip, w):
    rows = lambda width: pl.BlockSpec((BLOCK, width), lambda k: (k, 0))
    heads = pl.BlockSpec((HEADS, BLOCK), lambda k: (0, k))
    there = lambda v: pltpu.with_memory_space_constraint(v, pltpu.HBM)
    return pl.pallas_call(
        local_kernel,
        grid=(NBLK,),
        in_specs=[SMEM, rows(CH), rows(CH), rows(STATE), rows(STATE), heads, heads, whole((1, CH)), HBM],
        out_specs=(VMEM,) * 4 + (whole((BLOCK, CH)),) * 4 + (VMEM,),
        out_shape=(jax.ShapeDtypeStruct((BLOCK, CH), BF16),) * 4
        + (pltpu.HBM((BLOCK, CH), BF16),) * 4
        + (jax.ShapeDtypeStruct((CH, WA), BF16),),
        scratch_shapes=[
            pltpu.VMEM((BLOCK, CH), BF16),
            pltpu.VMEM((BLOCK, CH), BF16),
            pltpu.VMEM((STATE, CH), F32),
            pltpu.VMEM((PADH, HALF), F32),
            pltpu.VMEM((PADH, BLOCK), F32),
            pltpu.VMEM((PADH, BLOCK), F32),
            pltpu.SemaphoreType.DMA((1,)),
        ],
        cost_estimate=pl.CostEstimate(flops=int(3e9), bytes_accessed=0, transcendentals=0),
        compiler_params=pltpu.CompilerParams(vmem_limit_bytes=LIMIT),
        name="local_part",
    )(order, *(there(v) for v in (x, g, b, c, dt, ld)), skip, there(w))


def gated_rows(order, place, prefix, *args):
    outs = [((BLOCK, CH), BF16), ((8, HALF), F32)]
    scratch = []
    if prefix.ndim == 3:
        outs.append(((STATE, CH), BF16))
        scratch.append(((STATE, CH), F32))
    kernel = functools.partial(gate_kernel, place)
    return local_call(kernel, (order, prefix, *args), outs, scratch, 5e8, [SMEM] + [VMEM] * 5)


def product(rows, squares, w):
    width = w.shape[1]
    tall = TALL if width == WA else HALF
    outs = [((tall, width), BF16), ((HALF, width), F32)]
    return local_call(product_kernel, (rows, squares, w), outs, (), 2 * BLOCK * CH * width)


def middle(*args):
    gated = [((BLOCK, CH), BF16), ((8, HALF), F32)]
    outs = [((HALF, WB), BF16), ((HALF, WB), F32), *gated, *gated, ((CH, WB), BF16)]
    scratch = [gated[0], gated[0], 3]
    in_specs = [SMEM] + [VMEM] * 7 + [HBM] * 3
    return local_call(middle_kernel, args, outs, scratch, 2e9, in_specs)


def join(keep, got, *more):
    out = (TILES, 8, HALF) if got.shape[0] == TALL else keep.shape
    return local_call(join_kernel, (keep, got, *more), ((out, BF16),))[0]


def finish(devices, *args):
    kernel = functools.partial(finish_kernel, devices)
    out = ((HALF, D), BF16)
    scratch = [((HALF, HALF), F32), out, CHUNKS]
    return local_call(kernel, args, (out,), scratch, out_specs=[HBM])[0]


def after(value, earlier):
    return lax.optimization_barrier((value, earlier))[0]


def body(x, g, b, c, dt, ld, skip, gain, w):
    chips = lax.axis_size("x")
    chip, core = lax.axis_index("x"), lax.axis_index("c")
    up = [(i, (i + 1) % chips) for i in range(chips)]
    down = [(i, (i - 1) % chips) for i in range(chips)]
    swap = [(0, 1), (1, 0)]
    order = jnp.stack([core, (chip + 2) % chips, (chip + 3) % chips, (chip + 1) % chips, chip]).astype(jnp.int32)
    msg = local_state(x, b, dt.T, ld.T)
    msg = lax.all_to_all(msg, ("z", "y"), split_axis=0, concat_axis=0, tiled=True)
    skip_wide = jnp.repeat(skip, WIDTH)[None, :]
    *parts_of, w_a = local_part(order, x, g, b, c, dt.T, ld.T, skip_wide, w)
    far, left, right, own = (parts_of[2 * i : 2 * i + 2] for i in range(4))
    prefix = lax.all_to_all(seq_prefix(msg), ("z", "y"), split_axis=0, concat_axis=0, tiled=True)
    gain_row = gain.astype(F32)[None, :]

    rows, square, prefix = gated_rows(order, 1, prefix, gain_row, c, *far)
    send, far_keep_a = product(rows, square, w_a)
    far_got_a = lax.ppermute(send, "c", swap)
    send, far_keep_b, rows_left, square_left, rows_right, square_right, w_b = middle(
        order, prefix, gain_row, c, *left, after(rows, send), square, *right, w
    )
    far_got_b = lax.ppermute(send, "c", swap)
    far_a = join(after(far_keep_a, send), far_got_a, square)
    last = far_b = join(after(far_keep_b, far_a), far_got_b)
    far_a, far_b = lax.ppermute(far_a, "x", up), lax.ppermute(far_b, "x", down)

    send, left_keep_a = product(after(rows_left, last), square_left, w_a)
    left_got_a = lax.ppermute(send, "c", swap)
    send, right_keep_b = product(after(rows_right, send), square_right, w_b)
    right_got_b = lax.ppermute(send, "c", swap)
    last = left_a = join(after(left_keep_a, send), left_got_a, square_left)
    left_a = lax.ppermute(left_a, "x", down)
    last = right_b = join(after(right_keep_b, last), right_got_b)
    right_b = lax.ppermute(right_b, "x", up)
    send, right_keep_a = product(after(rows_right, last), square_right, w_a)
    right_got_a = lax.ppermute(send, "c", swap)
    send, left_keep_b = product(after(rows_left, send), square_left, w_b)
    left_got_b = lax.ppermute(send, "c", swap)
    last = right_a = join(after(right_keep_a, send), right_got_a, square_right, far_a)
    right_a = lax.ppermute(right_a, "x", up)
    last = left_b = join(after(left_keep_b, last), left_got_b, far_b)
    left_b = lax.ppermute(left_b, "x", down)

    rows, square = gated_rows(order, 4, after(prefix, last), gain_row, c, *own)
    send, keep_a = product(rows, square, w_a)
    got_a = lax.ppermute(send, "c", swap)
    send, keep_b = product(after(rows, send), square, w_b)
    got_b = lax.ppermute(send, "c", swap)
    outs = (((HALF, D), F32), ((8, HALF), F32))
    base, total = local_call(base_kernel, (square, keep_a, keep_b, got_a, got_b, left_a, right_b), outs)
    return finish(2 * chips, total, base, right_a, left_b)


def solution(mesh):
    torus = Mesh(mesh.devices.reshape(8, 4, 4, 2), ("z", "y", "x", "c"))
    seq, mp = ("z", "y"), ("x", "c")
    in_specs = (
        P(seq, mp),
        P(seq, mp),
        P(seq, None),
        P(seq, None),
        P(seq, mp),
        P(seq, mp),
        P(mp),
        P(mp),
        P(mp, None),
    )

    return jax.shard_map(body, mesh=torus, in_specs=in_specs, out_specs=P(seq + mp, None), check_vma=False)
```

```python
import functools

import jax
import jax.numpy as jnp
from jax import lax
from jax.experimental import pallas as pl
from jax.experimental.pallas import tpu as pltpu
from jax.sharding import Mesh
from jax.sharding import PartitionSpec as P


BLOCK = 256
HALF = 128
HEADS = 10
WIDTH = 64
CH = HEADS * WIDTH
STATE = 128
ROWS = 1024
NBLK = ROWS // BLOCK
SEQ_DEV = 32
PIECE = STATE // SEQ_DEV
D = 2560
WA = 1408
WB = D - WA
CHUNKS = 8
TILES = WA // HALF * (HALF // 8) + 1
PADH = 16
TALL = HALF + 8
LOG2E = 1.4426950408889634
F32 = jnp.float32
BF16 = jnp.bfloat16


def parts(value, count):
    out = []
    for _ in range(count):
        piece = value.astype(BF16)
        out.append(piece)
        value = value - piece.astype(F32)
    return out


def spread_matrix(count, tail):
    cols = CH + (HALF if tail else 0)
    row = lax.broadcasted_iota(jnp.int32, (PADH * count, cols), 0) % PADH
    col = lax.broadcasted_iota(jnp.int32, (PADH * count, cols), 1)
    head = jnp.where(col < CH, col // WIDTH, col - CH)
    return jnp.where(row == head, 1.0, 0.0).astype(BF16)


def spread(value, matrix, count):
    stacked = jnp.concatenate(parts(value, count), axis=0)
    return lax.dot_general(stacked, matrix, (((0,), (0,)), ((), ())), preferred_element_type=F32)


def triangle():
    row = lax.broadcasted_iota(jnp.int32, (BLOCK, BLOCK), 0)
    return jnp.where(row <= lax.broadcasted_iota(jnp.int32, (BLOCK, BLOCK), 1), 1.0, 0.0).astype(BF16)


def running_sums(value, upper):
    rows = value.shape[0]
    sums = jnp.dot(jnp.concatenate(parts(value, 3), axis=0), upper, preferred_element_type=F32)
    return sums[0:rows] + sums[rows : 2 * rows] + sums[2 * rows : 3 * rows]


def state_kernel(
    x_hbm, b_hbm, dt_hbm, ld_hbm, msg_ref, pad_ref, dtp_ref, run_ref, x_ref, b_ref, dt_ref, ld_ref,
    upper_ref, two_ref, sem
):
    copies = [pltpu.make_async_copy(ld_hbm, ld_ref, sem.at[0]), pltpu.make_async_copy(dt_hbm, dt_ref, sem.at[1])]
    for k in range(NBLK):
        rows = pl.ds(BLOCK * k, BLOCK)
        copies.append(pltpu.make_async_copy(x_hbm.at[rows, :], x_ref.at[rows, :], sem.at[2 + 2 * k]))
        copies.append(pltpu.make_async_copy(b_hbm.at[rows, :], b_ref.at[rows, :], sem.at[3 + 2 * k]))
    for copy in copies:
        copy.start()
    pad_ref[...] = jnp.zeros_like(pad_ref)
    dtp_ref[...] = jnp.zeros_like(dtp_ref)
    upper_ref[...] = triangle()
    two_ref[...] = spread_matrix(2, False)
    copies[0].wait()
    for k in range(NBLK):
        pad_ref[PADH * k : PADH * k + HEADS, :] = ld_ref[:, BLOCK * k : BLOCK * (k + 1)]
    levels = running_sums(pad_ref[...], upper_ref[...])
    closings = [levels[PADH * k : PADH * (k + 1), BLOCK - 1 : BLOCK] for k in range(NBLK)]
    tails = [jnp.zeros((PADH, 1), F32)]
    for k in reversed(range(NBLK)):
        tails.insert(0, tails[0] + closings[k])
    lane = lax.broadcasted_iota(jnp.int32, (PADH, HALF), 1)
    decay = spread(jnp.where(lane == 0, tails[0], 0.0), spread_matrix(3, True)[:, CH:], 3)[0:1, :]
    decays = jnp.concatenate([v.astype(F32) for v in parts(decay, 3)] + [jnp.zeros((1, HALF), F32)], axis=0)
    decays = decays.astype(BF16)
    two = two_ref[...]
    copies[1].wait()
    dtp_ref[0:HEADS, :] = dt_ref[...]
    wides = []
    for k in range(NBLK):
        weight = jnp.exp(tails[k] - levels[PADH * k : PADH * (k + 1)]) * dtp_ref[:, BLOCK * k : BLOCK * (k + 1)]
        wides.append(spread(weight, two, 2))
    for copy in copies[2:]:
        copy.wait()
    total = None
    for k in range(NBLK):
        weighted = (wides[k] * x_ref[BLOCK * k : BLOCK * (k + 1), :].astype(F32)).astype(BF16)
        own = lax.dot_general(
            b_ref[BLOCK * k : BLOCK * (k + 1), :], weighted, (((0,), (0,)), ((), ())), preferred_element_type=F32
        )
        total = own if total is None else total + own
    run_ref[...] = total
    for q in range(SEQ_DEV):
        msg_ref[q, :, 0:CH] = run_ref[PIECE * q : PIECE * (q + 1), :].astype(BF16)
        msg_ref[q, :, CH : CH + HALF] = decays


def prefix_kernel(msg_ref, out_hbm, dec_ref, out_ref, sem):
    for i in range(SEQ_DEV):
        for part in range(3):
            dec_ref[part, i : i + 1, :] = msg_ref[i, :, CH : CH + HALF].astype(F32)[part : part + 1]
    head = lax.broadcasted_iota(jnp.int32, (HALF, CH), 0)
    col = lax.broadcasted_iota(jnp.int32, (HALF, CH), 1)
    matrix = jnp.where(head == col // WIDTH, 1.0, 0.0).astype(BF16)
    logs = jnp.zeros((SEQ_DEV, CH), F32)
    for part in range(3):
        logs = logs + jnp.dot(dec_ref[part].astype(BF16), matrix, preferred_element_type=F32)
    decay = jnp.exp(logs)
    running = jnp.zeros((PIECE, CH), F32)
    group = SEQ_DEV // CHUNKS
    copies = []
    for i in range(SEQ_DEV):
        out_ref[i] = running.astype(BF16)
        running = decay[i : i + 1, :] * running + msg_ref[i, :, 0:CH].astype(F32)
        if i % group == group - 1:
            span = pl.ds(i + 1 - group, group)
            copies.append(pltpu.make_async_copy(out_ref.at[span], out_hbm.at[span], sem.at[i // group]))
            copies[-1].start()
    for copy in copies:
        copy.wait()


def local_kernel(
    idx_ref, x_ref, g_ref, b_ref, c_ref, dt_ref, ld_ref, skip_ref, w_hbm, far_gl_ref, far_fs_ref, left_gl_ref, left_fs_ref,
    right_gl_ref, right_fs_ref, own_gl_ref, own_fs_ref, w_ref,
    gl_ref, fs_ref, run_ref, lead_ref, pad_ref, dtp_ref, sem
):
    k = pl.program_id(0)
    fetch = pltpu.make_async_copy(w_hbm.at[:, pl.ds(0, WA)], w_ref, sem.at[0])

    @pl.when(k == 0)
    def _():
        fetch.start()
        run_ref[...] = jnp.zeros_like(run_ref)
        lead_ref[...] = jnp.zeros_like(lead_ref)
        pad_ref[...] = jnp.zeros_like(pad_ref)
        dtp_ref[...] = jnp.zeros_like(dtp_ref)

    pad_ref[0:HEADS, :] = ld_ref[...]
    dtp_ref[0:HEADS, :] = dt_ref[...]
    lev = running_sums(pad_ref[...], triangle())
    closing = lev[:, BLOCK - 1 : BLOCK]
    reader, writer = c_ref[...], b_ref[...]
    two = spread_matrix(2, False)
    lane = lax.broadcasted_iota(jnp.int32, (PADH, HALF), 1)
    table = jnp.where(lane == 0, jnp.exp(lead_ref[...]), jnp.where(lane == 1, jnp.exp(closing), 0.0))
    table = spread(table, spread_matrix(3, False), 3)
    lead = table[0:1, :]
    lead_ref[...] += closing
    grown = spread(jnp.exp(lev), two, 2)
    carry = jnp.dot(reader, run_ref[...].astype(BF16), preferred_element_type=F32)
    weight = spread(jnp.exp(closing - lev) * dtp_ref[...], two, 2)
    weighted = (weight * x_ref[...].astype(F32)).astype(BF16)
    own = lax.dot_general(writer, weighted, (((0,), (0,)), ((), ())), preferred_element_type=F32)
    run_ref[...] = table[1:2, :] * run_ref[...] + own
    lev2 = lev * LOG2E
    cols = jnp.transpose(lev2)
    rows = lev2[0:HEADS] - jnp.log(dt_ref[...]) * LOG2E
    inter = lax.dot_general(reader, writer, (((1,), (1,)), ((), ())), preferred_element_type=F32)
    causal = lax.broadcasted_iota(jnp.int32, (HALF, HALF), 0) >= lax.broadcasted_iota(jnp.int32, (HALF, HALF), 1)
    lane = lax.broadcasted_iota(jnp.int32, (HALF, HALF), 1) < WIDTH

    def score(head, r, s):
        gap = cols[HALF * r : HALF * (r + 1), head : head + 1] - rows[head : head + 1, HALF * s : HALF * (s + 1)]
        value = jnp.exp2(gap) * inter[HALF * r : HALF * (r + 1), HALF * s : HALF * (s + 1)]
        if r == s:
            value = jnp.where(causal, value, 0.0)
        return value.astype(BF16)

    for pair in range(HEADS // 2):
        lanes = slice(HALF * pair, HALF * (pair + 1))
        top_x = x_ref[0:HALF, lanes]
        low_x = x_ref[HALF:BLOCK, lanes]
        tops, lows = [], []
        for head in (2 * pair, 2 * pair + 1):
            tops.append(jnp.dot(score(head, 0, 0), top_x, preferred_element_type=F32))
            lows.append(
                jnp.dot(score(head, 1, 0), top_x, preferred_element_type=F32)
                + jnp.dot(score(head, 1, 1), low_x, preferred_element_type=F32)
            )
        for r, (even, odd), x_part in ((0, tops, top_x), (1, lows, low_x)):
            span = slice(HALF * r, HALF * (r + 1))
            mixed = (
                jnp.where(lane, even, odd)
                + grown[span, lanes] * carry[span, lanes]
                + skip_ref[:, lanes] * x_part.astype(F32)
            )
            gate = g_ref[span, lanes].astype(F32)
            gate = gate / (1.0 + jnp.exp(-gate))
            gl_ref[span, lanes] = (mixed * gate).astype(BF16)
            fs_ref[span, lanes] = (grown[span, lanes] * lead[:, lanes] * gate).astype(BF16)

    roles = (
        (far_gl_ref, far_fs_ref),
        (left_gl_ref, left_fs_ref),
        (right_gl_ref, right_fs_ref),
        (own_gl_ref, own_fs_ref),
    )
    for role, (to_gl_ref, to_fs_ref) in enumerate(roles):

        @pl.when(k == idx_ref[1 + role])
        def _():
            to_gl_ref[...] = gl_ref[...]
            to_fs_ref[...] = fs_ref[...]

    @pl.when(k == NBLK - 1)
    def _():
        fetch.wait()


def square_rows(total):
    rows = [piece.astype(F32) for piece in parts(total, 3)]
    return jnp.concatenate(rows + [jnp.zeros((8 - len(rows), HALF), F32)], axis=0).astype(BF16)


def squares_of(ref, first):
    return jnp.sum(ref[first : first + 8, 0:HALF].astype(F32), axis=0, keepdims=True)


def gate_block(place, idx_ref, state, gain, c_ref, gl_ref, fs_ref, rows_ref, square_ref):
    there = pl.ds(pl.multiple_of(idx_ref[place] * BLOCK, BLOCK), BLOCK)
    product = jnp.dot(c_ref[there, :], state, preferred_element_type=F32)
    gated = gl_ref[...].astype(F32) + fs_ref[...].astype(F32) * product
    sums = jnp.sum(gated * gated, axis=1, keepdims=True)
    value = (gated * gain).astype(BF16)
    square_ref[...] = jnp.zeros_like(square_ref)
    for half, n in enumerate((1 - idx_ref[0], idx_ref[0])):
        span = slice(HALF * half, HALF * (half + 1))
        rows_ref[pl.ds(pl.multiple_of(n * HALF, HALF), HALF), :] = value[span]
        square_ref[pl.ds(n, 1), :] = jnp.transpose(jnp.broadcast_to(sums[span], (HALF, HALF)))[0:1, :]


def gate_kernel(place, idx_ref, p_ref, gain_ref, c_ref, gl_ref, fs_ref, rows_ref, square_ref, *rest):
    if rest:
        p_out_ref, st_ref = rest
        for q in range(SEQ_DEV):
            st_ref[PIECE * q : PIECE * (q + 1), :] = p_ref[q].astype(F32)
        state = st_ref[...].astype(BF16)
        p_out_ref[...] = state
    else:
        state = p_ref[...]
    gate_block(place, idx_ref, state, gain_ref[...], c_ref, gl_ref, fs_ref, rows_ref, square_ref)


def product_kernel(rows_ref, square_ref, w_ref, send_ref, keep_ref):
    width = keep_ref.shape[1]
    rows = rows_ref[...]
    for base in range(0, width, BLOCK):
        cols = slice(base, min(base + BLOCK, width))
        value = jnp.dot(rows, w_ref[:, cols], preferred_element_type=F32)
        keep_ref[:, cols] = value[HALF:BLOCK]
        send_ref[0:HALF, cols] = value[0:HALF].astype(BF16)
    if send_ref.shape[0] == TALL:
        send_ref[HALF:TALL, 0:HALF] = square_rows(square_ref[0:1, :])
        send_ref[HALF:TALL, HALF:width] = jnp.zeros((TALL - HALF, width - HALF), BF16)


def middle_kernel(
    idx_ref, p_ref, gain_ref, c_ref, left_gl_ref, left_fs_ref, far_rows_ref, far_square_ref, right_gl_hbm, right_fs_hbm, w_hbm,
    send_ref, keep_ref, left_rows_ref, left_square_ref, right_rows_ref, right_square_ref, w_ref,
    right_gl_ref, right_fs_ref, sem
):
    fetches = [
        pltpu.make_async_copy(right_gl_hbm, right_gl_ref, sem.at[0]),
        pltpu.make_async_copy(right_fs_hbm, right_fs_ref, sem.at[1]),
        pltpu.make_async_copy(w_hbm.at[:, pl.ds(WA, WB)], w_ref, sem.at[2]),
    ]
    for fetch in fetches:
        fetch.start()
    state, gain = p_ref[...], gain_ref[...]
    gate_block(2, idx_ref, state, gain, c_ref, left_gl_ref, left_fs_ref, left_rows_ref, left_square_ref)
    fetches[0].wait()
    fetches[1].wait()
    gate_block(3, idx_ref, state, gain, c_ref, right_gl_ref, right_fs_ref, right_rows_ref, right_square_ref)
    fetches[2].wait()
    product_kernel(far_rows_ref, far_square_ref, w_ref, send_ref, keep_ref)


def tiles_of(width):
    per_row = width // HALF
    for n in range(HALF // 8 * per_row):
        yield n, n // per_row * 8, slice(n % per_row * HALF, (n % per_row + 1) * HALF)


def join_kernel(keep_ref, got_ref, *refs):
    out_ref = refs[-1]
    if got_ref.shape[0] == HALF:
        value = keep_ref[...] + got_ref[...].astype(F32)
        for ref in refs[:-1]:
            value = value + ref[...].astype(F32)
        out_ref[...] = value.astype(BF16)
        return
    square_ref, more = refs[0], refs[1:-1]
    for n, row, lanes in tiles_of(keep_ref.shape[1]):
        value = keep_ref[row : row + 8, lanes] + got_ref[row : row + 8, lanes].astype(F32)
        for ref in more:
            value = value + ref[n].astype(F32)
        out_ref[n] = value.astype(BF16)
    total = square_ref[1:2, :] + squares_of(got_ref, HALF)
    for ref in more:
        total = total + last_squares(ref)
    out_ref[TILES - 1] = square_rows(total)


def last_squares(ref):
    return jnp.sum(ref[TILES - 1].astype(F32), axis=0, keepdims=True)


def base_kernel(square_ref, ka_ref, kb_ref, ga_ref, gb_ref, la_ref, rb_ref, base_ref, total_ref):
    total = square_ref[1:2, :] + squares_of(ga_ref, HALF) + last_squares(la_ref)
    total_ref[...] = jnp.broadcast_to(total, total_ref.shape)
    for n, row, lanes in tiles_of(WA):
        span = slice(row, row + 8)
        base_ref[span, lanes] = ka_ref[span, lanes] + ga_ref[span, lanes].astype(F32) + la_ref[n].astype(F32)
    base_ref[:, WA:D] = kb_ref[...] + gb_ref[...].astype(F32) + rb_ref[...].astype(F32)


def finish_kernel(devices, total_ref, base_ref, ra_ref, lb_ref, out_hbm, scale_ref, out_ref, sem):
    total = total_ref[0:1, :] + last_squares(ra_ref)
    scale = lax.rsqrt(total / (CH * devices) + 1e-05)
    scale_ref[...] = jnp.transpose(jnp.broadcast_to(scale, (HALF, HALF)))
    copies = []
    group = HALF // CHUNKS
    for n, row, lanes in tiles_of(WA):
        span = slice(row, row + 8)
        out_ref[span, lanes] = ((base_ref[span, lanes] + ra_ref[n].astype(F32)) * scale_ref[span, 0:1]).astype(BF16)
        if lanes.stop == WA and (row + 8) % group == 0:
            span = slice(row + 8 - group, row + 8)
            value = base_ref[span, WA:D] + lb_ref[span, :].astype(F32)
            out_ref[span, WA:D] = (value * scale_ref[span, 0:1]).astype(BF16)
            span = pl.ds(row + 8 - group, group)
            copies.append(pltpu.make_async_copy(out_ref.at[span, :], out_hbm.at[span, :], sem.at[len(copies)]))
            copies[-1].start()
    for copy in copies:
        copy.wait()


VMEM = pl.BlockSpec(memory_space=pltpu.VMEM)
SMEM = pl.BlockSpec(memory_space=pltpu.SMEM)
HBM = pl.BlockSpec(memory_space=pltpu.HBM)
LIMIT = 24 * 1024 * 1024


def local_call(kernel, args, outs, scratch=(), flops=1e8, in_specs=None, out_specs=None):
    in_specs, out_specs = in_specs or [VMEM] * len(args), out_specs or [VMEM] * len(outs)
    args = [pltpu.with_memory_space_constraint(v, pltpu.HBM) if spec is HBM else v for v, spec in zip(args, in_specs)]
    return pl.pallas_call(
        kernel,
        in_specs=in_specs,
        out_specs=out_specs,
        out_shape=[
            pltpu.HBM(*out) if spec is HBM else jax.ShapeDtypeStruct(*out) for out, spec in zip(outs, out_specs)
        ],
        scratch_shapes=[pltpu.VMEM(*v) if isinstance(v, tuple) else pltpu.SemaphoreType.DMA((v,)) for v in scratch],
        cost_estimate=pl.CostEstimate(flops=int(flops), bytes_accessed=0, transcendentals=0),
        compiler_params=pltpu.CompilerParams(vmem_limit_bytes=LIMIT),
    )(*args)


def local_state(x, b, dt, ld):
    outs = (((SEQ_DEV, PIECE, CH + HALF), BF16),)
    scratch = [
        ((PADH * NBLK, BLOCK), F32),
        ((PADH, ROWS), F32),
        ((STATE, CH), F32),
        ((ROWS, CH), BF16),
        ((ROWS, STATE), BF16),
        ((HEADS, ROWS), F32),
        ((HEADS, ROWS), F32),
        ((BLOCK, BLOCK), BF16),
        ((2 * PADH, CH), BF16),
        2 + 2 * NBLK,
    ]
    return local_call(state_kernel, (x, b, dt, ld), outs, scratch, 1e9, [HBM] * 4)[0]


def seq_prefix(msg):
    outs = (((SEQ_DEV, PIECE, CH), BF16),)
    scratch = [((3, SEQ_DEV, HALF), F32), outs[0], CHUNKS]
    return local_call(prefix_kernel, (msg,), outs, scratch, out_specs=[HBM])[0]


def whole(shape):
    return pl.BlockSpec(shape, lambda *_: (0,) * len(shape))


def local_part(order, x, g, b, c, dt, ld, skip, w):
    rows = lambda width: pl.BlockSpec((BLOCK, width), lambda k: (k, 0))
    heads = pl.BlockSpec((HEADS, BLOCK), lambda k: (0, k))
    there = lambda v: pltpu.with_memory_space_constraint(v, pltpu.HBM)
    return pl.pallas_call(
        local_kernel,
        grid=(NBLK,),
        in_specs=[SMEM, rows(CH), rows(CH), rows(STATE), rows(STATE), heads, heads, whole((1, CH)), HBM],
        out_specs=(VMEM,) * 4 + (whole((BLOCK, CH)),) * 4 + (VMEM,),
        out_shape=(jax.ShapeDtypeStruct((BLOCK, CH), BF16),) * 4
        + (pltpu.HBM((BLOCK, CH), BF16),) * 4
        + (jax.ShapeDtypeStruct((CH, WA), BF16),),
        scratch_shapes=[
            pltpu.VMEM((BLOCK, CH), BF16),
            pltpu.VMEM((BLOCK, CH), BF16),
            pltpu.VMEM((STATE, CH), F32),
            pltpu.VMEM((PADH, HALF), F32),
            pltpu.VMEM((PADH, BLOCK), F32),
            pltpu.VMEM((PADH, BLOCK), F32),
            pltpu.SemaphoreType.DMA((1,)),
        ],
        cost_estimate=pl.CostEstimate(flops=int(3e9), bytes_accessed=0, transcendentals=0),
        compiler_params=pltpu.CompilerParams(vmem_limit_bytes=LIMIT),
        name="local_part",
    )(order, *(there(v) for v in (x, g, b, c, dt, ld)), skip, there(w))


def gated_rows(order, place, prefix, *args):
    outs = [((BLOCK, CH), BF16), ((8, HALF), F32)]
    scratch = []
    if prefix.ndim == 3:
        outs.append(((STATE, CH), BF16))
        scratch.append(((STATE, CH), F32))
    kernel = functools.partial(gate_kernel, place)
    return local_call(kernel, (order, prefix, *args), outs, scratch, 5e8, [SMEM] + [VMEM] * 5)


def product(rows, squares, w):
    width = w.shape[1]
    tall = TALL if width == WA else HALF
    outs = [((tall, width), BF16), ((HALF, width), F32)]
    return local_call(product_kernel, (rows, squares, w), outs, (), 2 * BLOCK * CH * width)


def middle(*args):
    gated = [((BLOCK, CH), BF16), ((8, HALF), F32)]
    outs = [((HALF, WB), BF16), ((HALF, WB), F32), *gated, *gated, ((CH, WB), BF16)]
    scratch = [gated[0], gated[0], 3]
    in_specs = [SMEM] + [VMEM] * 7 + [HBM] * 3
    return local_call(middle_kernel, args, outs, scratch, 2e9, in_specs)


def join(keep, got, *more):
    out = (TILES, 8, HALF) if got.shape[0] == TALL else keep.shape
    return local_call(join_kernel, (keep, got, *more), ((out, BF16),))[0]


def finish(devices, *args):
    kernel = functools.partial(finish_kernel, devices)
    out = ((HALF, D), BF16)
    scratch = [((HALF, HALF), F32), out, CHUNKS]
    return local_call(kernel, args, (out,), scratch, out_specs=[HBM])[0]


def after(value, earlier):
    return lax.optimization_barrier((value, earlier))[0]


def body(x, g, b, c, dt, ld, skip, gain, w):
    chips = lax.axis_size("x")
    chip, core = lax.axis_index("x"), lax.axis_index("c")
    up = [(i, (i + 1) % chips) for i in range(chips)]
    down = [(i, (i - 1) % chips) for i in range(chips)]
    swap = [(0, 1), (1, 0)]
    order = jnp.stack([core, (chip + 2) % chips, (chip + 3) % chips, (chip + 1) % chips, chip]).astype(jnp.int32)
    msg = local_state(x, b, dt.T, ld.T)
    msg = lax.all_to_all(msg, ("z", "y"), split_axis=0, concat_axis=0, tiled=True)
    skip_wide = jnp.repeat(skip, WIDTH)[None, :]
    *parts_of, w_a = local_part(order, x, g, b, c, dt.T, ld.T, skip_wide, w)
    far, left, right, own = (parts_of[2 * i : 2 * i + 2] for i in range(4))
    prefix = lax.all_to_all(seq_prefix(msg), ("z", "y"), split_axis=0, concat_axis=0, tiled=True)
    gain_row = gain.astype(F32)[None, :]

    rows, square, prefix = gated_rows(order, 1, prefix, gain_row, c, *far)
    send, far_keep_a = product(rows, square, w_a)
    far_got_a = lax.ppermute(send, "c", swap)
    send, far_keep_b, rows_left, square_left, rows_right, square_right, w_b = middle(
        order, prefix, gain_row, c, *left, after(rows, send), square, *right, w
    )
    far_got_b = lax.ppermute(send, "c", swap)
    far_a = join(after(far_keep_a, send), far_got_a, square)
    last = far_b = join(after(far_keep_b, far_a), far_got_b)
    far_a, far_b = lax.ppermute(far_a, "x", up), lax.ppermute(far_b, "x", down)

    send, left_keep_a = product(after(rows_left, last), square_left, w_a)
    left_got_a = lax.ppermute(send, "c", swap)
    send, right_keep_b = product(after(rows_right, send), square_right, w_b)
    right_got_b = lax.ppermute(send, "c", swap)
    last = left_a = join(after(left_keep_a, send), left_got_a, square_left)
    left_a = lax.ppermute(left_a, "x", down)
    last = right_b = join(after(right_keep_b, last), right_got_b)
    right_b = lax.ppermute(right_b, "x", up)
    send, right_keep_a = product(after(rows_right, last), square_right, w_a)
    right_got_a = lax.ppermute(send, "c", swap)
    send, left_keep_b = product(after(rows_left, send), square_left, w_b)
    left_got_b = lax.ppermute(send, "c", swap)
    last = right_a = join(after(right_keep_a, send), right_got_a, square_right, far_a)
    right_a = lax.ppermute(right_a, "x", up)
    last = left_b = join(after(left_keep_b, last), left_got_b, far_b)
    left_b = lax.ppermute(left_b, "x", down)

    rows, square = gated_rows(order, 4, after(prefix, last), gain_row, c, *own)
    send, keep_a = product(rows, square, w_a)
    got_a = lax.ppermute(send, "c", swap)
    send, keep_b = product(after(rows, send), square, w_b)
    got_b = lax.ppermute(send, "c", swap)
    outs = (((HALF, D), F32), ((8, HALF), F32))
    base, total = local_call(base_kernel, (square, keep_a, keep_b, got_a, got_b, left_a, right_b), outs)
    return finish(2 * chips, total, base, right_a, left_b)


def solution(mesh):
    torus = Mesh(mesh.devices.reshape(8, 4, 4, 2), ("z", "y", "x", "c"))
    seq, mp = ("z", "y"), ("x", "c")
    in_specs = (
        P(seq, mp),
        P(seq, mp),
        P(seq, None),
        P(seq, None),
        P(seq, mp),
        P(seq, mp),
        P(mp),
        P(mp),
        P(mp, None),
    )

    return jax.shard_map(body, mesh=torus, in_specs=in_specs, out_specs=P(seq + mp, None), check_vma=False)
```
